32 devices in a mesh: gx: 8 (over z, x), gy: 4 (over y, core).
Axes of the slice: x: 2, y: 2, z: 4, core: 2. Of those that a mesh axis runs over, the one named last changes fastest.
Arguments:
- ambient_compactness: float32 [16, 8, 6, 6, 6, 128], P('gx', 'gy'), may hold values from 0.5 to 2
- ambient_flow_knots: float32 [16, 8, 3, 6, 6, 6, 128], P('gx', 'gy'), may hold values from -5 to 5
- ambient_hotness_knots: float32 [16, 8, 6, 6, 6, 128], P('gx', 'gy'), may hold values from 0.5 to 2
- parent_subdomain: int32 [8192], P(('gx', 'gy')), may hold values from 0 to 4095, as said below
- parcel_membership: int32 [8192], P(('gx', 'gy')), may hold values from 1 to 128
- particle_basis_coefficients: float32 [8192, 3, 6, 128], P(('gx', 'gy')), may hold values from -0.1 to 0.4
- parcel_velocities_list: float32 [8192, 3, 128], P(('gx', 'gy')), may hold values from -3 to 3
- parcel_breadth: float32 [8192, 128], P(('gx', 'gy')), may hold values from 0.5 to 2
- parcel_hotness: float32 [8192, 128], P(('gx', 'gy')), may hold values from 0.5 to 2
Outputs:
- residual: float32 [16, 8, 5, 6, 6, 6, 128], P('gx', 'gy')
The draws below stay inside these ranges and needn't reach their ends.
Inputs may be any that keep to these rules, and one draw needn't show every extreme that they name: parent_subdomain[b] = s * 512 + l names element l of streamwise slab s within bin b's own spanwise slab. Of the 256 bins of one device at most 64 have their host on any one streamwise slab; the same three cyclically neighbouring slabs take exactly 64 bins from every device.
All inputs are finite; a program needn't handle non-finite values.
Results may differ from the reference program's by a relative error of at most 0.0003.
Values sent between devices are 32-bit elements; how exact they have to be, the bound alone decides.
No kernel may reach another device: no remote copies, remote signals or barrier semaphores. Data moves between devices by JAX's collectives and lax.ppermute only.
A program may use at most 128 MiB of HBM per device.

```python
import math
import jax
import jax.numpy as jnp
import numpy as np
from jax import lax

EXD = 2
EYD = 2
HEIGHT_EXTENT = 128
CELLS_OF_DEVICE = 256
ORDER_KNOTS = 6
CELL_PLACES = 128
SLABS = 8
SPANS = 4
STREAMWISE_COUNT = 16
SPANWISE_EXTENT = 8
E_DEV = 512
CAP = 64
OVERALL_CELLS = 8192


def draw_parent_subdomain(key, part):
    base_key = jax.random.fold_in(key, 7)
    first_key, spread_key, order_key, local_key = jax.random.split(base_key, 4)
    blocks = OVERALL_CELLS // CELLS_OF_DEVICE
    curtain = jax.random.randint(first_key, (), 0, SLABS)
    position = jnp.arange(CELLS_OF_DEVICE, dtype=jnp.int32)
    scatter = jax.random.randint(spread_key, (blocks, CELLS_OF_DEVICE), 0, SLABS - 3)
    offset = jnp.where(position[None, :] < 3 * CAP, position[None, :] // CAP, 3 + scatter)
    slab_id = (curtain + offset) % SLABS
    order_rows = jax.vmap(lambda sub_key: jax.random.permutation(sub_key, CELLS_OF_DEVICE))(jax.random.split(order_key, blocks))
    slab_id = jnp.take_along_axis(slab_id, order_rows, axis=1)
    local_elem = jax.random.randint(local_key, (blocks, CELLS_OF_DEVICE), 0, E_DEV)
    return (slab_id * E_DEV + local_elem).reshape(OVERALL_CELLS).astype(jnp.int32)


def touch_ends(entries, key, smallest, top_value):
    extent = entries.shape
    place = [jax.random.randint(jax.random.fold_in(key, axis), (), 0, extent[axis]) for axis in range(len(extent))]
    entries = entries.at[tuple(place)].set(smallest)
    longest = extent.index(max(extent))
    place[longest] = (place[longest] + 1) % extent[longest]
    return entries.at[tuple(place)].set(top_value)


def shard_levels(rng, dims, pieces, smallest, largest):
    gain, own = 1.0, jax.random.fold_in(rng, 6)
    for dim, parts in pieces:
        steps = jnp.exp(jax.random.uniform(jax.random.fold_in(own, dim), (parts,), jnp.float32, smallest / len(pieces), largest / len(pieces)))
        gain = gain * jnp.repeat(steps, dims[dim] // parts).reshape([-1 if axis == dim else 1 for axis in range(len(dims))])
    return gain


def normal_values(stream_key, dims, spread, reach, pieces=(), held_as=jnp.bfloat16):
    result = jax.random.normal(stream_key, dims, jnp.float32) * spread
    if len(pieces) > 0:
        result = shard_levels(stream_key, dims, pieces, -0.22, 0.18) * result
    return jnp.clip(result, min=-reach, max=reach).astype(held_as)


def setup_inputs(seed: int = 0) -> dict:
    key_list = jax.random.split(jax.random.key(seed), 10)
    ambient_compactness = jnp.clip(jnp.exp(math.log(2.0) - 1.3862944 * jax.random.uniform(key_list[0], (STREAMWISE_COUNT, SPANWISE_EXTENT, ORDER_KNOTS, ORDER_KNOTS, ORDER_KNOTS, HEIGHT_EXTENT), jnp.float32) ** shard_levels(key_list[0], (STREAMWISE_COUNT, SPANWISE_EXTENT, ORDER_KNOTS, ORDER_KNOTS, ORDER_KNOTS, HEIGHT_EXTENT), ((0, 8), (1, 4)), -0.2, 0.2)), 0.5, 2.0)
    ambient_flow_knots = normal_values(key_list[1], (STREAMWISE_COUNT, SPANWISE_EXTENT, 3, ORDER_KNOTS, ORDER_KNOTS, ORDER_KNOTS, HEIGHT_EXTENT), 1.0, 5.0, ((0, 8), (1, 4)), jnp.float32)
    ambient_hotness_knots = jnp.clip(jnp.exp(math.log(2.0) - 1.3862944 * jax.random.uniform(key_list[2], (STREAMWISE_COUNT, SPANWISE_EXTENT, ORDER_KNOTS, ORDER_KNOTS, ORDER_KNOTS, HEIGHT_EXTENT), jnp.float32) ** shard_levels(key_list[2], (STREAMWISE_COUNT, SPANWISE_EXTENT, ORDER_KNOTS, ORDER_KNOTS, ORDER_KNOTS, HEIGHT_EXTENT), ((0, 8), (1, 4)), -0.2, 0.2)), 0.5, 2.0)
    parent_subdomain = draw_parent_subdomain(jax.random.fold_in(key_list[9], 71), 0)
    parcel_membership = touch_ends(jax.random.randint(key_list[4], (OVERALL_CELLS,), 1, CELL_PLACES + 1), jax.random.fold_in(key_list[4], 1), 1, CELL_PLACES).astype(jnp.int32)
    particle_basis_coefficients = jnp.clip(-0.1 + 0.5 * jax.random.uniform(key_list[5], (OVERALL_CELLS, 3, ORDER_KNOTS, CELL_PLACES), jnp.float32) ** shard_levels(key_list[5], (OVERALL_CELLS, 3, ORDER_KNOTS, CELL_PLACES), ((0, 32),), -0.2, 0.2), -0.1, 0.4)
    parcel_velocities_list = normal_values(key_list[6], (OVERALL_CELLS, 3, CELL_PLACES), 0.5, 3.0, ((0, 32),), jnp.float32)
    parcel_breadth = jnp.clip(jnp.exp(math.log(2.0) - 1.3862944 * jax.random.uniform(key_list[7], (OVERALL_CELLS, CELL_PLACES), jnp.float32) ** shard_levels(key_list[7], (OVERALL_CELLS, CELL_PLACES), ((0, 32),), -0.2, 0.2)), 0.5, 2.0)
    parcel_hotness = jnp.clip(jnp.exp(math.log(2.0) - 1.3862944 * jax.random.uniform(key_list[8], (OVERALL_CELLS, CELL_PLACES), jnp.float32) ** shard_levels(key_list[8], (OVERALL_CELLS, CELL_PLACES), ((0, 32),), -0.2, 0.2)), 0.5, 2.0)
    return {"ambient_compactness": ambient_compactness, "ambient_flow_knots": ambient_flow_knots, "ambient_hotness_knots": ambient_hotness_knots, "parent_subdomain": parent_subdomain, "parcel_membership": parcel_membership, "particle_basis_coefficients": particle_basis_coefficients, "parcel_velocities_list": parcel_velocities_list, "parcel_breadth": parcel_breadth, "parcel_hotness": parcel_hotness}


SPECIFIC_CP = 2.5
MU_GAS = 0.2
CONDUCTANCE = 0.2
PRANDTL = 0.72

def gll_tables():
    root_seven = math.sqrt(7.0)
    outer_node = math.sqrt(1.0 / 3.0 + 2.0 * root_seven / 21.0)
    inner_node = math.sqrt(1.0 / 3.0 - 2.0 * root_seven / 21.0)
    points = np.array([-1.0, -outer_node, -inner_node, inner_node, outer_node, 1.0])
    outer_weight = (14.0 - root_seven) / 30.0
    inner_weight = (14.0 + root_seven) / 30.0
    quadrature = np.array([1.0 / 15.0, outer_weight, inner_weight, inner_weight, outer_weight, 1.0 / 15.0])
    barycentric = np.ones(6)
    for row_at in range(6):
        for col_at in range(6):
            if col_at != row_at:
                barycentric[row_at] = barycentric[row_at] / (points[row_at] - points[col_at])
    matrix = np.zeros((6, 6))
    for row_at in range(6):
        for col_at in range(6):
            if col_at != row_at:
                matrix[row_at, col_at] = barycentric[col_at] / barycentric[row_at] / (points[row_at] - points[col_at])
        matrix[row_at, row_at] = -np.sum(matrix[row_at])
    volume = quadrature[:, None, None] * quadrature[None, :, None] * quadrature[None, None, :]
    return (jnp.asarray(matrix, dtype=jnp.float32), jnp.asarray(volume, dtype=jnp.float32))

def apply_along(knot_readings, matrix, direction):
    einsum_forms = ('ai,...ijkz->...ajkz', 'aj,...ijkz->...iakz', 'ak,...ijkz->...ijaz')
    return jnp.einsum(einsum_forms[direction], matrix, knot_readings, precision=lax.Precision.HIGHEST)

def ambient_coupling(compactness_measure, flow_vectors, hotness_listing):
    matrix, volume = gll_tables()
    thermodynamic_push = compactness_measure * hotness_listing
    momentum = compactness_measure[..., None, :, :, :, :] * flow_vectors
    thermal_forcing = compactness_measure * (SPECIFIC_CP * hotness_listing + 0.5 * lax.optimization_barrier(jnp.sum(flow_vectors * flow_vectors, axis=-5)))
    divergence = None
    for direction in range(3):
        speed_dir = flow_vectors[..., direction, :, :, :, :]
        stress = momentum * speed_dir[..., None, :, :, :, :]
        stress = stress.at[..., direction, :, :, :, :].add(thermodynamic_push)
        flux_dir = jnp.concatenate([momentum[..., direction:direction + 1, :, :, :, :], stress, ((thermal_forcing + thermodynamic_push) * speed_dir)[..., None, :, :, :, :]], axis=-5)
        term_dir = apply_along(flux_dir, matrix, direction)
        divergence = term_dir if divergence is None else divergence + term_dir
    return -volume[:, :, :, None] * divergence

def cell_feedback(parent_subdomain_condition, lagrange_factors, grain_speed, parcel_breadths, parcel_hotness_advanced, tally_occupancy):
    bin_rows = lagrange_factors.shape[0]
    slot_count = lagrange_factors.shape[-1]
    basis_table = lagrange_factors[:, 0, :, None, None, :] * lagrange_factors[:, 1, None, :, None, :] * lagrange_factors[:, 2, None, None, :, :]
    basis_table = basis_table.reshape(bin_rows, 216, slot_count)
    stacked = parent_subdomain_condition.reshape(bin_rows, 5, 216)
    computed_readings = jnp.einsum('bcn,bns->bcs', stacked, basis_table, precision=lax.Precision.HIGHEST)
    gas_density = computed_readings[:, 0]
    gas_velocity = computed_readings[:, 1:4]
    queried_ambient_hotness = computed_readings[:, 4]
    relative = gas_velocity - grain_speed
    reynolds_sq = (gas_density * parcel_breadths / MU_GAS) ** 2 * lax.optimization_barrier(jnp.sum(relative * relative, axis=1)) + 1.0
    drag_factor = 1.0 + 0.15 * jnp.power(reynolds_sq, 0.3435)
    drag_force = 3.0 * math.pi * MU_GAS * (parcel_breadths * drag_factor)[:, None, :] * relative
    transfer_quotient = 2.0 + 0.6 * PRANDTL ** (1.0 / 3.0) * jnp.power(reynolds_sq, 0.25)
    hotness_tendency = math.pi * CONDUCTANCE * parcel_breadths * transfer_quotient * (queried_ambient_hotness - parcel_hotness_advanced)
    coupled_work = lax.optimization_barrier(jnp.sum(drag_force * grain_speed, axis=1)) + hotness_tendency
    live_slots = (jnp.arange(slot_count, dtype=jnp.int32)[None, :] < tally_occupancy[:, None]).astype(jnp.float32)
    coupling = jnp.concatenate([drag_force, coupled_work[:, None, :]], axis=1) * live_slots[:, None, :]
    return jnp.einsum('bqs,bns->bqn', coupling, basis_table, precision=lax.Precision.HIGHEST)

def reference(ambient_compactness, ambient_flow_knots, ambient_hotness_knots, parent_subdomain, parcel_membership, particle_basis_coefficients, parcel_velocities_list, parcel_breadth, parcel_hotness):
    ambient_fraction = lax.map(lambda stratum_batch: ambient_coupling(stratum_batch[0], stratum_batch[1], stratum_batch[2]), (ambient_compactness, ambient_flow_knots, ambient_hotness_knots))
    tile_amount_overall = OVERALL_CELLS // CELLS_OF_DEVICE

    def lone_tile(given_arrays):
        tile_ordinal, owning_mesh_ordinal, tally_occupancy, lagrange_factors, flow_vectors, parcel_breadths, hotness_listing = given_arrays
        slab_id = owning_mesh_ordinal // E_DEV
        local_elem = owning_mesh_ordinal % E_DEV
        subdomain_streamwise = slab_id * EXD + local_elem // (EYD * HEIGHT_EXTENT)
        subdomain_spanwise = tile_ordinal % SPANS * EYD + local_elem // HEIGHT_EXTENT % EYD
        subdomain_height = local_elem % HEIGHT_EXTENT
        parent_subdomain_condition = jnp.concatenate([ambient_compactness[subdomain_streamwise, subdomain_spanwise, :, :, :, subdomain_height][:, None], ambient_flow_knots[subdomain_streamwise, subdomain_spanwise, :, :, :, :, subdomain_height], ambient_hotness_knots[subdomain_streamwise, subdomain_spanwise, :, :, :, subdomain_height][:, None]], axis=1)
        mapped_forcing = cell_feedback(parent_subdomain_condition, lagrange_factors, flow_vectors, parcel_breadths, hotness_listing, tally_occupancy)
        return (mapped_forcing, subdomain_streamwise, subdomain_spanwise, subdomain_height)
    mapped_forcing, subdomain_streamwise, subdomain_spanwise, subdomain_height = lax.map(lone_tile, (jnp.arange(tile_amount_overall, dtype=jnp.int32), parent_subdomain.reshape(tile_amount_overall, CELLS_OF_DEVICE), parcel_membership.reshape(tile_amount_overall, CELLS_OF_DEVICE), particle_basis_coefficients.reshape((tile_amount_overall, CELLS_OF_DEVICE) + particle_basis_coefficients.shape[1:]), parcel_velocities_list.reshape((tile_amount_overall, CELLS_OF_DEVICE) + parcel_velocities_list.shape[1:]), parcel_breadth.reshape((tile_amount_overall, CELLS_OF_DEVICE) + parcel_breadth.shape[1:]), parcel_hotness.reshape((tile_amount_overall, CELLS_OF_DEVICE) + parcel_hotness.shape[1:])))
    drag_loads = jnp.zeros((STREAMWISE_COUNT, SPANWISE_EXTENT, 4, 6, 6, 6, HEIGHT_EXTENT), jnp.float32)
    drag_loads = drag_loads.at[subdomain_streamwise.reshape(-1), subdomain_spanwise.reshape(-1), :, :, :, :, subdomain_height.reshape(-1)].add(mapped_forcing.reshape(-1, 4, 6, 6, 6))
    knot_readings = ambient_fraction - jnp.concatenate([jnp.zeros_like(drag_loads[:, :, :1]), drag_loads], axis=2)
    lower_face = knot_readings[:, :, :, 0]
    upper_face = knot_readings[:, :, :, 5]
    zero_plane = jnp.zeros_like(lower_face[:1])
    next_lower = jnp.concatenate([lower_face[1:], zero_plane], axis=0)
    prev_upper = jnp.concatenate([zero_plane, upper_face[:-1]], axis=0)
    knot_readings = knot_readings.at[:, :, :, 5].set(upper_face + next_lower).at[:, :, :, 0].set(lower_face + prev_upper)
    lower_face = knot_readings[:, :, :, :, 0]
    upper_face = knot_readings[:, :, :, :, 5]
    next_lower = jnp.roll(lower_face, -1, axis=1)
    prev_upper = jnp.roll(upper_face, 1, axis=1)
    knot_readings = knot_readings.at[:, :, :, :, 5].set(upper_face + next_lower).at[:, :, :, :, 0].set(lower_face + prev_upper)
    lower_face = knot_readings[..., 0, :]
    upper_face = knot_readings[..., 5, :]
    next_lower = jnp.roll(lower_face, -1, axis=-1)
    prev_upper = jnp.roll(upper_face, 1, axis=-1)
    return knot_readings.at[..., 5, :].set(upper_face + next_lower).at[..., 0, :].set(lower_face + prev_upper)
```

```python
import functools
import math

import jax
import jax.numpy as jnp
import numpy as np
from jax import lax
from jax.experimental import pallas as pl
from jax.experimental.pallas import tpu as pltpu
from jax.sharding import PartitionSpec as P

SPECIFIC_CP = 2.5
MU_GAS = 0.2
CONDUCTANCE = 0.2
PRANDTL = 0.72

NODES = 216
LANES = 128
CHUNKS = 2
F32 = jnp.float32
BF16 = jnp.bfloat16
I32 = jnp.int32
NT = (((1,), (1,)), ((), ()))


def gll_operator():
    root_seven = math.sqrt(7.0)
    outer_node = math.sqrt(1.0 / 3.0 + 2.0 * root_seven / 21.0)
    inner_node = math.sqrt(1.0 / 3.0 - 2.0 * root_seven / 21.0)
    points = np.array([-1.0, -outer_node, -inner_node, inner_node, outer_node, 1.0])
    outer_weight = (14.0 - root_seven) / 30.0
    inner_weight = (14.0 + root_seven) / 30.0
    w = np.array([1.0 / 15.0, outer_weight, inner_weight, inner_weight, outer_weight, 1.0 / 15.0])
    bary = np.ones(6)
    for r in range(6):
        for c in range(6):
            if c != r:
                bary[r] = bary[r] / (points[r] - points[c])
    dm = np.zeros((6, 6))
    for r in range(6):
        for c in range(6):
            if c != r:
                dm[r, c] = bary[c] / bary[r] / (points[r] - points[c])
        dm[r, r] = -np.sum(dm[r])
    eye = np.eye(6)
    volume = np.kron(np.kron(w, w), w)
    blocks = [
        np.kron(np.kron(dm, eye), eye),
        np.kron(np.kron(eye, dm), eye),
        np.kron(np.kron(eye, eye), dm),
    ]
    return (-volume[:, None] * np.concatenate(blocks, axis=1)).astype(np.float32)


def halves(x):
    hi = x.astype(BF16)
    return hi, (x - hi.astype(F32)).astype(BF16)


def thirds(x):
    hi = x.astype(BF16)
    rest = x - hi.astype(F32)
    mid = rest.astype(BF16)
    return hi, mid, (rest - mid.astype(F32)).astype(BF16)


def pick(x, weights):
    hi, lo = halves(x)
    return jnp.dot(hi, weights, preferred_element_type=F32) + jnp.dot(
        lo, weights, preferred_element_type=F32
    )


def iota(shape, dim):
    return lax.broadcasted_iota(I32, shape, dim)


def sorted_places(ids, elems, groups):
    rows, bins = ids.shape
    shift = elems.bit_length() - 1
    assert elems == 1 << shift
    slab = jnp.right_shift(ids, shift)
    upper = (iota((bins, bins), 0) < iota((bins, bins), 1)).astype(F32).astype(BF16)
    places, firsts = [], []
    group_of = iota((groups, bins), 0)
    for d in range(rows):
        mine = jnp.broadcast_to(slab[d : d + 1], (groups, bins))
        hit = (mine == group_of).astype(F32)
        earlier = jnp.dot(hit.astype(BF16), upper, preferred_element_type=F32)
        first = jnp.sum((mine < group_of).astype(F32), axis=1, keepdims=True)
        places.append(jnp.sum(hit * (earlier + first), axis=0, keepdims=True).astype(I32))
        firsts.append(first.astype(I32))
    return places, slab, firsts


def state_columns(rho_ref, vel_ref, hot_ref, ex, ey):
    out = []
    for q in range(5):
        cols = []
        for x in range(ex):
            for y in range(ey):
                if q == 0 or q == 4:
                    ref, base = (rho_ref if q == 0 else hot_ref), x * NODES * ey + y
                else:
                    ref, base = vel_ref, (x * 3 + q - 1) * NODES * ey + y
                cols.append(ref[pl.ds(base, NODES, stride=ey), :])
        out.append(cols)
    return out


def gather_kernel(c, elems, ex, ey, me_ref, ids_ref, rho_ref, vel_ref, hot_ref, out_ref, req_ref, work):
    groups, bins = ids_ref.shape
    me = me_ref[0]
    cap = out_ref.shape[2] // 4
    slots = groups * cap
    ids = ids_ref[...]
    places, slab, firsts = sorted_places(ids, elems, groups)
    elem = jnp.bitwise_and(ids, elems - 1)
    sub = iota((LANES, bins), 0)
    slot_of = iota((slots, bins), 0)
    row_table = jnp.zeros((LANES, slots), F32)
    col_table = jnp.zeros((slots, LANES), F32)
    for d in range(groups):
        place = places[d]
        first = jnp.sum(
            jnp.where(iota((groups, 1), 0) == me, firsts[d], 0).astype(F32), axis=0, keepdims=True
        ).astype(I32)
        begin = jnp.right_shift(first - c + 1, 1)
        here = (slab[d : d + 1] == me) & (jnp.bitwise_and(place, 1) == c)
        slot = jnp.where(here, jnp.right_shift(place, 1) - begin + d * cap, -1)
        match = (jnp.broadcast_to(slot, (slots, bins)) == slot_of).astype(F32).astype(BF16)
        e = jnp.broadcast_to(elem[d : d + 1], (LANES, bins))
        parts = jnp.where(
            sub == 0,
            jnp.bitwise_and(e, 255),
            jnp.where(sub == 1, jnp.right_shift(e, 8), jnp.where(sub == 2, 1, 0)),
        )
        parts = parts.astype(F32).astype(BF16)
        row_table += lax.dot_general(parts, match, NT, preferred_element_type=F32)
        col_table += lax.dot_general(match, parts, NT, preferred_element_type=F32)
    wanted = jnp.where(row_table[2:3] > 0.5, row_table[0:1] + 256.0 * row_table[1:2], -1.0).astype(I32)
    wanted_col = jnp.where(
        col_table[:, 2:3] > 0.5, col_table[:, 0:1] + 256.0 * col_table[:, 1:2], -1.0
    ).astype(I32)
    req_ref[...] = jnp.broadcast_to(wanted_col, (slots, LANES))
    onehot = (jnp.broadcast_to(wanted, (elems, slots)) == iota((elems, slots), 0)).astype(F32).astype(BF16)
    state = state_columns(rho_ref, vel_ref, hot_ref, ex, ey)
    for q in range(5):
        work[q * NODES : (q + 1) * NODES, :] = pick(jnp.concatenate(state[q], axis=1), onehot)
    rows = out_ref.shape[1]
    pad = 4 * rows - 5 * NODES
    work[5 * NODES : 4 * rows, :] = jnp.zeros((pad, slots), F32)
    lane_group = iota((rows, LANES), 1) // cap
    for tile in range(slots // LANES):
        block = [
            work[g * rows : (g + 1) * rows, tile * LANES : (tile + 1) * LANES] for g in range(4)
        ]
        for at in range(4):
            total = None
            for g in range(4):
                turn = ((g - at) % 4) * cap
                moved = block[g] if turn == 0 else pltpu.roll(block[g], turn, 1)
                total = moved if total is None else jnp.where(lane_group == g, moved, total)
            out_ref[tile * 4 + at] = total


def arrange_kernel(elems, groups, ids_ref, count_ref, basis_ref, vel_ref, breadth_ref, hot_ref, out_ref, live_ref):
    bins = ids_ref.shape[1]
    half = bins // CHUNKS
    places, _, _ = sorted_places(ids_ref[...], elems, groups)
    place = places[0]
    target = jnp.bitwise_and(place, 1) * half + jnp.right_shift(place, 1)
    move = (jnp.broadcast_to(target, (bins, bins)) == iota((bins, bins), 0)).astype(F32).astype(BF16)
    count = jnp.broadcast_to(count_ref[...], (8, bins)).astype(F32).astype(BF16)
    live = lax.dot_general(count, move, NT, preferred_element_type=F32)
    for c in range(CHUNKS):
        live_ref[c] = live[:, c * half : (c + 1) * half].astype(I32)
    sources = [basis_ref.at[m] for m in range(18)] + [vel_ref.at[m] for m in range(3)]
    sources += [breadth_ref, hot_ref]
    for m, source in enumerate(sources):
        hi, mid, lo = thirds(source[...])
        moved = (
            jnp.dot(move, hi, preferred_element_type=F32)
            + jnp.dot(move, mid, preferred_element_type=F32)
            + jnp.dot(move, lo, preferred_element_type=F32)
        )
        for c in range(CHUNKS):
            out_ref[c, m] = moved[c * half : (c + 1) * half].T


def fluid_kernel(ex, ey, op_ref, rho_ref, vel_ref, hot_ref, out_ref, lead, flow, push):
    state = state_columns(rho_ref, vel_ref, hot_ref, ex, ey)
    for at in range(ex * ey):
        lanes = slice(at * LANES, (at + 1) * LANES)
        rho, hot = state[0][at], state[4][at]
        u = [state[1 + d][at] for d in range(3)]
        p = rho * hot
        energy = rho * (SPECIFIC_CP * hot + 0.5 * (u[0] * u[0] + u[1] * u[1] + u[2] * u[2]))
        push[:, lanes] = p
        lead[0, :, lanes] = rho
        lead[4, :, lanes] = energy + p
        for d in range(3):
            flow[d, :, lanes] = u[d]
            lead[1 + d, :, lanes] = rho * u[d]

    def component(q, _):
        parts = []
        for d in range(3):
            extra = jnp.where(q == d + 1, 1.0, 0.0).astype(F32)
            parts.append(lead[q] * flow[d] + extra * push[...])
        flux = jnp.concatenate(parts, axis=0)
        out_ref[q] = jnp.dot(
            op_ref[...], flux, preferred_element_type=F32, precision=lax.Precision.HIGHEST
        )
        return 0

    lax.fori_loop(0, 5, component, 0)


def particle_kernel(c, firsts_ref, recv_ref, data_ref, live_ref, out_ref, host, work, force):
    groups, rows, _ = recv_ref.shape
    cap = LANES // 4
    slots_t = data_ref.shape[1]
    width = data_ref.shape[2]
    begins = [jnp.right_shift(firsts_ref[g] - c + 1, 1) for g in range(groups + 1)]

    row = iota((LANES, width), 0)
    col = iota((LANES, width), 1)
    slot = jnp.bitwise_and(row, cap - 1)
    lane_group = jnp.right_shift(row, cap.bit_length() - 1)
    bases = [(col - slot == begins[d]) & (col < begins[d + 1]) for d in range(groups)]
    got_hi, got_lo = halves(jnp.concatenate([recv_ref[d] for d in range(groups)], axis=1))
    for g in range(4):
        weights = jnp.concatenate(
            [(bases[d] & (lane_group == g)).astype(F32).astype(BF16) for d in range(groups)], axis=0
        )
        host[g * rows : (g + 1) * rows, :] = jnp.dot(
            got_hi, weights, preferred_element_type=F32
        ) + jnp.dot(got_lo, weights, preferred_element_type=F32)

    step = 16
    live = live_ref[0:1, :]

    def sample(tb, _):
        at = pl.ds(pl.multiple_of(tb * step, step), step)
        b0 = [data_ref[i, at, :] for i in range(6)]
        b1 = [data_ref[6 + i, at, :] for i in range(6)]
        b2 = [data_ref[12 + i, at, :] for i in range(6)]
        sampled = []
        for q in range(5):
            over_i = None
            for i in range(6):
                over_j = None
                for j in range(6):
                    over_k = None
                    for k in range(6):
                        n = q * NODES + i * 36 + j * 6 + k
                        term = host[n : n + 1, :] * b2[k]
                        over_k = term if over_k is None else over_k + term
                    term = over_k * b1[j]
                    over_j = term if over_j is None else over_j + term
                term = over_j * b0[i]
                over_i = term if over_i is None else over_i + term
            sampled.append(over_i)
        v = [data_ref[18 + d, at, :] for d in range(3)]
        breadth, hot = data_ref[21, at, :], data_ref[22, at, :]
        rel = [sampled[1 + d] - v[d] for d in range(3)]
        ratio = sampled[0] * breadth * (1.0 / MU_GAS)
        reynolds = ratio * ratio * (rel[0] * rel[0] + rel[1] * rel[1] + rel[2] * rel[2]) + 1.0
        drag = (3.0 * math.pi * MU_GAS) * (breadth * (1.0 + 0.15 * jnp.exp(0.3435 * jnp.log(reynolds))))
        transfer = 2.0 + 0.6 * PRANDTL ** (1.0 / 3.0) * jnp.sqrt(jnp.sqrt(reynolds))
        heat = (math.pi * CONDUCTANCE) * breadth * transfer * (sampled[4] - hot)
        on = iota((step, width), 0) + tb * step < live
        pull = [drag * rel[d] for d in range(3)]
        power = pull[0] * v[0] + pull[1] * v[1] + pull[2] * v[2] + heat
        for r, value in enumerate(pull + [power]):
            force[r, at, :] = jnp.where(on, value, 0.0)
        return 0

    lax.fori_loop(0, slots_t // step, sample, 0)

    def project(ij, _):
        i, j = ij // 6, ij % 6
        acc = [[None] * 6 for _ in range(4)]
        for tb in range(slots_t // 8):
            at = slice(tb * 8, tb * 8 + 8)
            both = data_ref[i, at, :] * data_ref[6 + j, at, :]
            b2 = [data_ref[12 + k, at, :] for k in range(6)]
            for r in range(4):
                g = force[r, at, :] * both
                for k in range(6):
                    term = g * b2[k]
                    acc[r][k] = term if acc[r][k] is None else acc[r][k] + term
        for r in range(4):
            for k in range(6):
                work[pl.ds(r * NODES + ij * 6 + k, 1), :] = jnp.sum(acc[r][k], axis=0, keepdims=True)
        return 0

    lax.fori_loop(0, 36, project, 0)

    row = iota((width, LANES), 0)
    col = iota((width, LANES), 1)
    slot = jnp.bitwise_and(col, cap - 1)
    lane_group = jnp.right_shift(col, cap.bit_length() - 1)
    give_hi, give_lo = halves(
        jnp.concatenate([work[r * NODES : (r + 1) * NODES, :] for r in range(4)], axis=1)
    )
    for d in range(groups):
        base = (row - slot == begins[d]) & (row < begins[d + 1])
        weights = jnp.concatenate(
            [(base & (lane_group == r)).astype(F32).astype(BF16) for r in range(4)], axis=0
        )
        out_ref[d] = jnp.dot(give_hi, weights, preferred_element_type=F32) + jnp.dot(
            give_lo, weights, preferred_element_type=F32
        )


def collect(recv_ref, req_ref, elems):
    groups, rows, _ = recv_ref.shape
    cap = LANES // 4
    got = jnp.concatenate([recv_ref[d] for d in range(groups)], axis=1)
    lane_group = jnp.right_shift(jnp.bitwise_and(iota(got.shape, 1), LANES - 1), cap.bit_length() - 1)
    weights = []
    for d in range(groups):
        want = req_ref[d * cap : (d + 1) * cap, :]
        parts = [(want == iota(want.shape, 1) + t * LANES) for t in range(elems // LANES)]
        part = jnp.concatenate([p.astype(F32).astype(BF16) for p in parts], axis=1)
        weights += [part] * 4
    weights = jnp.concatenate(weights, axis=0)
    hi, lo = halves(got)
    zero = jnp.zeros_like(hi)
    out = []
    for r in range(4):
        mine = lane_group == r
        out.append(
            jnp.dot(jnp.where(mine, hi, zero), weights, preferred_element_type=F32)
            + jnp.dot(jnp.where(mine, lo, zero), weights, preferred_element_type=F32)
        )
    return out


def load_kernel(recv_ref, req_ref, fluid_ref, out_ref):
    loads = collect(recv_ref, req_ref, fluid_ref.shape[2])
    out_ref[0] = fluid_ref[0]
    for r in range(4):
        out_ref[1 + r] = fluid_ref[1 + r] - loads[r]


def join_kernel(ex, ey, recv_ref, req_ref, part_ref, out_ref, xlo_ref, xhi_ref, ylo_ref, yhi_ref, corner_ref):
    loads = collect(recv_ref, req_ref, part_ref.shape[2])
    out_ref[0] = part_ref[0]
    for r in range(4):
        out_ref[1 + r] = part_ref[1 + r] - loads[r]
    wide = ey * LANES
    for q in range(5):
        for x in range(ex - 1):
            a, b = slice(x * wide, (x + 1) * wide), slice((x + 1) * wide, (x + 2) * wide)
            total = out_ref[q, 180:216, a] + out_ref[q, 0:36, b]
            out_ref[q, 180:216, a] = total
            out_ref[q, 0:36, b] = total
        for x in range(ex):
            for y in range(ey - 1):
                base = x * wide + y * LANES
                a, b = slice(base, base + LANES), slice(base + LANES, base + 2 * LANES)
                for i in range(6):
                    total = out_ref[q, 36 * i + 30 : 36 * i + 36, a] + out_ref[q, 36 * i : 36 * i + 6, b]
                    out_ref[q, 36 * i + 30 : 36 * i + 36, a] = total
                    out_ref[q, 36 * i : 36 * i + 6, b] = total
        last = (ex - 1) * wide
        xlo_ref[q] = out_ref[q, 0:36, 0:wide]
        xhi_ref[q] = out_ref[q, 180:216, last : last + wide]
        for x in range(ex):
            dst = slice(x * LANES, (x + 1) * LANES)
            lo = slice(x * wide, x * wide + LANES)
            hi = slice((x + 1) * wide - LANES, (x + 1) * wide)
            for i in range(6):
                ylo_ref[q, 6 * i : 6 * i + 6, dst] = out_ref[q, 36 * i : 36 * i + 6, lo]
                yhi_ref[q, 6 * i : 6 * i + 6, dst] = out_ref[q, 36 * i + 30 : 36 * i + 36, hi]
        for at, (x, y) in enumerate(((0, 0), (0, 1), (1, 0), (1, 1))):
            start = 180 * x + 30 * y
            lanes = x * last + y * (wide - LANES)
            corner_ref[at, q] = jnp.zeros((8, LANES), F32)
            corner_ref[at, q, 0:6, :] = out_ref[q, start : start + 6, lanes : lanes + LANES]


def finish_kernel(ex, ey, part_ref, xl_ref, xr_ref, yl_ref, yr_ref, c00_ref, c01_ref, c10_ref, c11_ref, out_ref, work):
    for q in range(5):
        for at in range(ex * ey):
            work[at] = part_ref[q, :, at * LANES : (at + 1) * LANES]
        for y in range(ey):
            lanes = slice(y * LANES, (y + 1) * LANES)
            work[y, 0:36, :] += xl_ref[q, :, lanes]
            work[(ex - 1) * ey + y, 180:216, :] += xr_ref[q, :, lanes]
        for x in range(ex):
            lanes = slice(x * LANES, (x + 1) * LANES)
            for i in range(6):
                work[x * ey, 36 * i : 36 * i + 6, :] += yl_ref[q, 6 * i : 6 * i + 6, lanes]
                work[x * ey + ey - 1, 36 * i + 30 : 36 * i + 36, :] += yr_ref[q, 6 * i : 6 * i + 6, lanes]
        for ref, x, y in ((c00_ref, 0, 0), (c01_ref, 0, 1), (c10_ref, 1, 0), (c11_ref, 1, 1)):
            start = 180 * x + 30 * y
            work[x * (ex - 1) * ey + y * (ey - 1), start : start + 6, :] += ref[q, 0:6, :]
        for x in range(ex):
            for y in range(ey):
                at = x * ey + y
                lower = work[at, pl.ds(0, 36, stride=6), :]
                upper = work[at, pl.ds(5, 36, stride=6), :]
                work[at, pl.ds(5, 36, stride=6), :] = upper + pltpu.roll(lower, LANES - 1, 1)
                work[at, pl.ds(0, 36, stride=6), :] = lower + pltpu.roll(upper, 1, 1)
                out_ref[pl.ds((x * 5 + q) * NODES * ey + y, NODES, stride=ey), :] = work[at]


def call(kernel, out_shape, scratch=(), smem=0, flops=0, operands=()):
    n = len(operands)
    in_specs = [
        pl.BlockSpec(memory_space=pltpu.SMEM if at < smem else pltpu.VMEM) for at in range(n)
    ]
    outs = jax.tree.map(lambda s: pl.BlockSpec(memory_space=pltpu.VMEM), out_shape)
    moved = sum(x.size * 4 for x in operands)
    return pl.pallas_call(
        kernel,
        out_shape=out_shape,
        in_specs=in_specs,
        out_specs=outs,
        scratch_shapes=list(scratch),
        cost_estimate=pl.CostEstimate(flops=flops, bytes_accessed=moved, transcendentals=0),
        compiler_params=pltpu.CompilerParams(vmem_limit_bytes=48 << 20),
    )(*operands)


def shape(*dims, dtype=F32):
    return jax.ShapeDtypeStruct(dims, dtype)


def shards(rho, flow, hot, parent, count, basis, speed, breadth, heat):
    ex, ey, height = rho.shape[0], rho.shape[1], rho.shape[-1]
    elems = ex * ey * height
    groups, spans = lax.axis_size("gx"), lax.axis_size("gy")
    bins = parent.shape[0]
    half = bins // CHUNKS
    cap = bins // 4 // CHUNKS
    slots_t = basis.shape[-1]
    rows = -(-5 * NODES // 32) * 8
    me = lax.axis_index("gx").astype(I32).reshape(1)

    ids = lax.all_gather(parent, "gx")
    own = parent.reshape(1, bins)
    firsts = jnp.sum(
        (own // elems < jnp.arange(groups + 1, dtype=I32)[:, None]).astype(I32), axis=1
    )
    rho_v = rho.transpose(0, 2, 3, 4, 1, 5).reshape(-1, height)
    flow_v = flow.transpose(0, 2, 3, 4, 5, 1, 6).reshape(-1, height)
    hot_v = hot.transpose(0, 2, 3, 4, 1, 5).reshape(-1, height)
    basis_v = basis.transpose(1, 2, 0, 3).reshape(18, bins, slots_t)
    speed_v = speed.transpose(1, 0, 2)

    sent, wanted = [], []
    for c in range(CHUNKS):
        wire, req = call(
            functools.partial(gather_kernel, c, elems, ex, ey),
            (shape(groups, rows, 4 * cap), shape(groups * cap, LANES, dtype=I32)),
            [pltpu.VMEM((4 * rows, groups * cap), F32)],
            smem=1,
            flops=10_000_000,
            operands=(me, ids, rho_v, flow_v, hot_v),
        )
        sent.append(wire)
        wanted.append(req)
    exchange = functools.partial(lax.all_to_all, axis_name="gx", split_axis=0, concat_axis=0, tiled=True)
    states = [exchange(wire) for wire in sent]
    data, live = call(
        functools.partial(arrange_kernel, elems, groups),
        (shape(CHUNKS, 23, slots_t, half), shape(CHUNKS, 8, half, dtype=I32)),
        flops=10_000_000,
        operands=(own, count.reshape(1, bins), basis_v, speed_v, breadth, heat),
    )
    fluid = call(
        functools.partial(fluid_kernel, ex, ey),
        shape(5, NODES, elems),
        [
            pltpu.VMEM((5, NODES, elems), F32),
            pltpu.VMEM((3, NODES, elems), F32),
            pltpu.VMEM((NODES, elems), F32),
        ],
        flops=10_000_000,
        operands=(jnp.asarray(gll_operator()), rho_v, flow_v, hot_v),
    )
    given = []
    for c in range(CHUNKS):
        wire = call(
            functools.partial(particle_kernel, c),
            shape(groups, NODES, 4 * cap),
            [
                pltpu.VMEM((4 * rows, half), F32),
                pltpu.VMEM((4 * NODES, half), F32),
                pltpu.VMEM((4, slots_t, half), F32),
            ],
            smem=1,
            flops=20_000_000,
            operands=(firsts, states[c], data[c], live[c]),
        )
        given.append(exchange(wire))
    part = call(
        load_kernel, shape(5, NODES, elems), flops=5_000_000, operands=(given[0], wanted[0], fluid)
    )
    wide = ey * height
    part, xlo, xhi, ylo, yhi, corner = call(
        functools.partial(join_kernel, ex, ey),
        (
            shape(5, NODES, elems),
            shape(5, 36, wide),
            shape(5, 36, wide),
            shape(5, 36, ex * height),
            shape(5, 36, ex * height),
            shape(4, 5, 8, height),
        ),
        flops=5_000_000,
        operands=(given[1], wanted[1], part),
    )
    up_x = [(i, i + 1) for i in range(groups - 1)]
    down_x = [(i + 1, i) for i in range(groups - 1)]
    up_y = [(i, (i + 1) % spans) for i in range(spans)]
    down_y = [((i + 1) % spans, i) for i in range(spans)]

    def diagonal(xs, ys):
        return [(a * spans + c, b * spans + d) for a, b in xs for c, d in ys]

    both = ("gx", "gy")
    halos = (
        lax.ppermute(xhi, "gx", up_x),
        lax.ppermute(xlo, "gx", down_x),
        lax.ppermute(yhi, "gy", up_y),
        lax.ppermute(ylo, "gy", down_y),
        lax.ppermute(corner[3], both, diagonal(up_x, up_y)),
        lax.ppermute(corner[2], both, diagonal(up_x, down_y)),
        lax.ppermute(corner[1], both, diagonal(down_x, up_y)),
        lax.ppermute(corner[0], both, diagonal(down_x, down_y)),
    )
    out = call(
        functools.partial(finish_kernel, ex, ey),
        shape(ex * 5 * NODES * ey, height),
        [pltpu.VMEM((ex * ey, NODES, height), F32)],
        flops=5_000_000,
        operands=(part,) + halos,
    )
    out = out.reshape(ex, 5, 6, 6, 6, ey, height)
    return out.transpose(0, 5, 1, 2, 3, 4, 6)


def solution(mesh):
    placed = (
        P("gx", "gy", None, None, None, None),
        P("gx", "gy", None, None, None, None, None),
        P("gx", "gy", None, None, None, None),
        P(("gx", "gy")),
        P(("gx", "gy")),
        P(("gx", "gy"), None, None, None),
        P(("gx", "gy"), None, None),
        P(("gx", "gy"), None),
        P(("gx", "gy"), None),
    )
    return jax.shard_map(
        shards,
        mesh=mesh,
        in_specs=placed,
        out_specs=P("gx", "gy", None, None, None, None, None),
        check_vma=False,
    )
```

```python
import functools
import math

import jax
import jax.numpy as jnp
import numpy as np
from jax import lax
from jax.experimental import pallas as pl
from jax.experimental.pallas import tpu as pltpu
from jax.sharding import PartitionSpec as P


SPECIFIC_CP = 2.5
MU_GAS = 0.2
CONDUCTANCE = 0.2
PRANDTL = 0.72

NODES = 216
LANES = 128
CHUNKS = 2
F32 = jnp.float32
BF16 = jnp.bfloat16
I32 = jnp.int32
NT = (((1,), (1,)), ((), ()))


def gll_operator():
    root_seven = math.sqrt(7.0)
    outer_node = math.sqrt(1.0 / 3.0 + 2.0 * root_seven / 21.0)
    inner_node = math.sqrt(1.0 / 3.0 - 2.0 * root_seven / 21.0)
    points = np.array([-1.0, -outer_node, -inner_node, inner_node, outer_node, 1.0])
    outer_weight = (14.0 - root_seven) / 30.0
    inner_weight = (14.0 + root_seven) / 30.0
    w = np.array([1.0 / 15.0, outer_weight, inner_weight, inner_weight, outer_weight, 1.0 / 15.0])
    bary = np.ones(6)
    for r in range(6):
        for c in range(6):
            if c != r:
                bary[r] = bary[r] / (points[r] - points[c])
    dm = np.zeros((6, 6))
    for r in range(6):
        for c in range(6):
            if c != r:
                dm[r, c] = bary[c] / bary[r] / (points[r] - points[c])
        dm[r, r] = -np.sum(dm[r])
    eye = np.eye(6)
    volume = np.kron(np.kron(w, w), w)
    blocks = [
        np.kron(np.kron(dm, eye), eye),
        np.kron(np.kron(eye, dm), eye),
        np.kron(np.kron(eye, eye), dm),
    ]
    return (-volume[:, None] * np.concatenate(blocks, axis=1)).astype(np.float32)


def halves(x):
    hi = x.astype(BF16)
    return hi, (x - hi.astype(F32)).astype(BF16)


def thirds(x):
    hi = x.astype(BF16)
    rest = x - hi.astype(F32)
    mid = rest.astype(BF16)
    return hi, mid, (rest - mid.astype(F32)).astype(BF16)


def iota(shape, dim):
    return lax.broadcasted_iota(I32, shape, dim)


def sorted_places(ids, elems, groups):
    rows, bins = ids.shape
    shift = elems.bit_length() - 1
    assert elems == 1 << shift
    slab = jnp.right_shift(ids, shift)
    upper = (iota((bins, bins), 0) < iota((bins, bins), 1)).astype(F32).astype(BF16)
    places, firsts = [], []
    group_of = iota((groups, bins), 0)
    for d in range(rows):
        mine = jnp.broadcast_to(slab[d : d + 1], (groups, bins))
        hit = (mine == group_of).astype(F32)
        earlier = jnp.dot(hit.astype(BF16), upper, preferred_element_type=F32)
        first = jnp.sum((mine < group_of).astype(F32), axis=1, keepdims=True)
        places.append(jnp.sum(hit * (earlier + first), axis=0, keepdims=True).astype(I32))
        firsts.append(first.astype(I32))
    return places, slab, firsts


def state_columns(rho_ref, vel_ref, hot_ref, ex, ey):
    out = []
    for q in range(5):
        cols = []
        for x in range(ex):
            for y in range(ey):
                if q == 0 or q == 4:
                    ref, base = (rho_ref if q == 0 else hot_ref), x * NODES * ey + y
                else:
                    ref, base = vel_ref, (x * 3 + q - 1) * NODES * ey + y
                cols.append(ref[pl.ds(base, NODES, stride=ey), :])
        out.append(cols)
    return out


def split_kernel(ex, ey, rho_ref, vel_ref, hot_ref, hi_ref, lo_ref):
    state = state_columns(rho_ref, vel_ref, hot_ref, ex, ey)
    for q in range(5):
        hi, lo = halves(jnp.concatenate(state[q], axis=1))
        hi_ref[q * NODES : (q + 1) * NODES, :] = hi
        lo_ref[q * NODES : (q + 1) * NODES, :] = lo


def block_device(c, s, me, groups, sign):
    return s if c == 0 else lax.rem(me + sign * s + groups, groups)


def block_view(refs, s):
    return refs[0].at[s] if len(refs) == 1 else refs[s]


def gather_kernel(c, elems, groups, me_ref, ids_ref, hi_ref, lo_ref, after_ref, *refs):
    out_refs, (req_ref, work) = refs[:-2], refs[-2:]
    bins = ids_ref.shape[1]
    me = me_ref[0]
    rows = out_refs[0].shape[-2]
    cap = LANES // 4
    slots = groups * cap
    ids = jnp.concatenate(
        [ids_ref[pl.ds(block_device(c, s, me, groups, 1), 1), :] for s in range(groups)], axis=0
    )
    places, slab, firsts = sorted_places(ids, elems, groups)
    elem = jnp.bitwise_and(ids, elems - 1)
    sub = iota((LANES, bins), 0)
    slot_of = iota((slots, bins), 0)
    row_table = jnp.zeros((LANES, slots), F32)
    col_table = jnp.zeros((slots, LANES), F32)
    for d in range(groups):
        place = places[d]
        first = jnp.sum(
            jnp.where(iota((groups, 1), 0) == me, firsts[d], 0).astype(F32), axis=0, keepdims=True
        ).astype(I32)
        begin = jnp.right_shift(first - c + 1, 1)
        here = (slab[d : d + 1] == me) & (jnp.bitwise_and(place, 1) == c)
        slot = jnp.where(here, jnp.right_shift(place, 1) - begin + d * cap, -1)
        match = (jnp.broadcast_to(slot, (slots, bins)) == slot_of).astype(F32).astype(BF16)
        e = jnp.broadcast_to(elem[d : d + 1], (LANES, bins))
        parts = jnp.where(
            sub == 0,
            jnp.bitwise_and(e, 255),
            jnp.where(sub == 1, jnp.right_shift(e, 8), jnp.where(sub == 2, 1, 0)),
        )
        parts = parts.astype(F32).astype(BF16)
        row_table += lax.dot_general(parts, match, NT, preferred_element_type=F32)
        col_table += lax.dot_general(match, parts, NT, preferred_element_type=F32)
    wanted = jnp.where(row_table[2:3] > 0.5, row_table[0:1] + 256.0 * row_table[1:2], -1.0).astype(I32)
    wanted_col = jnp.where(
        col_table[:, 2:3] > 0.5, col_table[:, 0:1] + 256.0 * col_table[:, 1:2], -1.0
    ).astype(I32)
    req_ref[...] = jnp.broadcast_to(wanted_col, (slots, LANES))
    onehot = (jnp.broadcast_to(wanted, (elems, slots)) == iota((elems, slots), 0)).astype(F32).astype(BF16)
    work[0 : 5 * NODES, :] = jnp.dot(
        hi_ref[...], onehot, preferred_element_type=F32
    ) + jnp.dot(lo_ref[...], onehot, preferred_element_type=F32)
    pad = 4 * rows - 5 * NODES
    work[5 * NODES : 4 * rows, :] = jnp.zeros((pad, slots), F32)
    lane_group = iota((rows, LANES), 1) // cap
    for tile in range(slots // LANES):
        block = [
            work[g * rows : (g + 1) * rows, tile * LANES : (tile + 1) * LANES] for g in range(4)
        ]
        for at in range(4):
            total = None
            for g in range(4):
                turn = ((g - at) % 4) * cap
                moved = block[g] if turn == 0 else pltpu.roll(block[g], turn, 1)
                total = moved if total is None else jnp.where(lane_group == g, moved, total)
            block_view(out_refs, tile * 4 + at)[...] = total


def arrange_kernel(elems, groups, ids_ref, count_ref, basis_ref, vel_ref, breadth_ref, hot_ref, *out_refs):
    bins = ids_ref.shape[1]
    half = bins // CHUNKS
    places, _, _ = sorted_places(ids_ref[...], elems, groups)
    place = places[0]
    target = jnp.bitwise_and(place, 1) * half + jnp.right_shift(place, 1)
    move = (jnp.broadcast_to(target, (bins, bins)) == iota((bins, bins), 0)).astype(F32).astype(BF16)
    count = jnp.broadcast_to(count_ref[...], (8, bins)).astype(F32).astype(BF16)
    live = lax.dot_general(count, move, NT, preferred_element_type=F32)
    for c in range(CHUNKS):
        out_refs[CHUNKS + c][...] = live[:, c * half : (c + 1) * half].astype(I32)
    sources = [basis_ref.at[m] for m in range(18)] + [vel_ref.at[m] for m in range(3)]
    sources += [breadth_ref, hot_ref]
    for m, source in enumerate(sources):
        hi, mid, lo = thirds(source[...])
        moved = (
            jnp.dot(move, hi, preferred_element_type=F32)
            + jnp.dot(move, mid, preferred_element_type=F32)
            + jnp.dot(move, lo, preferred_element_type=F32)
        )
        for c in range(CHUNKS):
            out_refs[c][m] = moved[c * half : (c + 1) * half].T


def fluid_kernel(ex, ey, op_ref, rho_ref, vel_ref, hot_ref, out_ref, lead, flow, push):
    state = state_columns(rho_ref, vel_ref, hot_ref, ex, ey)
    for at in range(ex * ey):
        lanes = slice(at * LANES, (at + 1) * LANES)
        rho, hot = state[0][at], state[4][at]
        u = [state[1 + d][at] for d in range(3)]
        p = rho * hot
        energy = rho * (SPECIFIC_CP * hot + 0.5 * (u[0] * u[0] + u[1] * u[1] + u[2] * u[2]))
        push[:, lanes] = p
        lead[0, :, lanes] = rho
        lead[4, :, lanes] = energy + p
        for d in range(3):
            flow[d, :, lanes] = u[d]
            lead[1 + d, :, lanes] = rho * u[d]

    def component(q, _):
        parts = []
        for d in range(3):
            extra = jnp.where(q == d + 1, 1.0, 0.0).astype(F32)
            parts.append(lead[q] * flow[d] + extra * push[...])
        flux = jnp.concatenate(parts, axis=0)
        out_ref[q] = jnp.dot(
            op_ref[...], flux, preferred_element_type=F32, precision=lax.Precision.HIGHEST
        )
        return 0

    lax.fori_loop(0, 5, component, 0)


def particle_kernel(c, groups, me_ref, firsts_ref, data_ref, live_ref, after_ref, *refs):
    host, work, force = refs[-3:]
    blocks = 1 if c == 0 else groups
    recv_refs, out_refs = refs[:blocks], refs[blocks:-3]
    rows = recv_refs[0].shape[-2]
    cap = LANES // 4
    me = me_ref[0]
    slots_t = data_ref.shape[1]
    width = data_ref.shape[2]
    begins, ends = [], []
    for s in range(groups):
        g = block_device(c, s, me, groups, -1)
        begins.append(jnp.right_shift(firsts_ref[g] - c + 1, 1))
        ends.append(jnp.right_shift(firsts_ref[g + 1] - c + 1, 1))

    row = iota((LANES, width), 0)
    col = iota((LANES, width), 1)
    slot = jnp.bitwise_and(row, cap - 1)
    lane_group = jnp.right_shift(row, cap.bit_length() - 1)
    bases = [(col - slot == begins[d]) & (col < ends[d]) for d in range(groups)]
    got_hi, got_lo = halves(jnp.concatenate([block_view(recv_refs, s)[...] for s in range(groups)], axis=1))
    for g in range(4):
        weights = jnp.concatenate(
            [(bases[d] & (lane_group == g)).astype(F32).astype(BF16) for d in range(groups)], axis=0
        )
        host[g * rows : (g + 1) * rows, :] = jnp.dot(
            got_hi, weights, preferred_element_type=F32
        ) + jnp.dot(got_lo, weights, preferred_element_type=F32)

    step = 16
    live = live_ref[0:1, :]

    def sample(tb, _):
        at = pl.ds(pl.multiple_of(tb * step, step), step)
        b0 = [data_ref[i, at, :] for i in range(6)]
        b1 = [data_ref[6 + i, at, :] for i in range(6)]
        b2 = [data_ref[12 + i, at, :] for i in range(6)]
        sampled = []
        for q in range(5):
            over_i = None
            for i in range(6):
                over_j = None
                for j in range(6):
                    over_k = None
                    for k in range(6):
                        n = q * NODES + i * 36 + j * 6 + k
                        term = host[n : n + 1, :] * b2[k]
                        over_k = term if over_k is None else over_k + term
                    term = over_k * b1[j]
                    over_j = term if over_j is None else over_j + term
                term = over_j * b0[i]
                over_i = term if over_i is None else over_i + term
            sampled.append(over_i)
        v = [data_ref[18 + d, at, :] for d in range(3)]
        breadth, hot = data_ref[21, at, :], data_ref[22, at, :]
        rel = [sampled[1 + d] - v[d] for d in range(3)]
        ratio = sampled[0] * breadth * (1.0 / MU_GAS)
        reynolds = ratio * ratio * (rel[0] * rel[0] + rel[1] * rel[1] + rel[2] * rel[2]) + 1.0
        drag = (3.0 * math.pi * MU_GAS) * (breadth * (1.0 + 0.15 * jnp.exp(0.3435 * jnp.log(reynolds))))
        transfer = 2.0 + 0.6 * PRANDTL ** (1.0 / 3.0) * jnp.sqrt(jnp.sqrt(reynolds))
        heat = (math.pi * CONDUCTANCE) * breadth * transfer * (sampled[4] - hot)
        on = iota((step, width), 0) + tb * step < live
        pull = [drag * rel[d] for d in range(3)]
        power = pull[0] * v[0] + pull[1] * v[1] + pull[2] * v[2] + heat
        for r, value in enumerate(pull + [power]):
            force[r, at, :] = jnp.where(on, value, 0.0)
        return 0

    lax.fori_loop(0, slots_t // step, sample, 0)

    def project(ij, _):
        i, j = ij // 6, ij % 6
        acc = [[None] * 6 for _ in range(4)]
        for tb in range(slots_t // 8):
            at = slice(tb * 8, tb * 8 + 8)
            both = data_ref[i, at, :] * data_ref[6 + j, at, :]
            b2 = [data_ref[12 + k, at, :] for k in range(6)]
            for r in range(4):
                g = force[r, at, :] * both
                for k in range(6):
                    term = g * b2[k]
                    acc[r][k] = term if acc[r][k] is None else acc[r][k] + term
        for r in range(4):
            for k in range(6):
                work[pl.ds(r * NODES + ij * 6 + k, 1), :] = jnp.sum(acc[r][k], axis=0, keepdims=True)
        return 0

    lax.fori_loop(0, 36, project, 0)

    row = iota((width, LANES), 0)
    col = iota((width, LANES), 1)
    slot = jnp.bitwise_and(col, cap - 1)
    lane_group = jnp.right_shift(col, cap.bit_length() - 1)
    give_hi, give_lo = halves(
        jnp.concatenate([work[r * NODES : (r + 1) * NODES, :] for r in range(4)], axis=1)
    )
    for d in range(groups):
        base = (row - slot == begins[d]) & (row < ends[d])
        weights = jnp.concatenate(
            [(base & (lane_group == r)).astype(F32).astype(BF16) for r in range(4)], axis=0
        )
        block_view(out_refs, d)[...] = jnp.dot(give_hi, weights, preferred_element_type=F32) + jnp.dot(
            give_lo, weights, preferred_element_type=F32
        )


def collect(recv_refs, groups, req_ref, elems):
    cap = LANES // 4
    got = jnp.concatenate([block_view(recv_refs, s)[...] for s in range(groups)], axis=1)
    lane_group = jnp.right_shift(jnp.bitwise_and(iota(got.shape, 1), LANES - 1), cap.bit_length() - 1)
    weights = []
    for d in range(groups):
        want = req_ref[d * cap : (d + 1) * cap, :]
        parts = [(want == iota(want.shape, 1) + t * LANES) for t in range(elems // LANES)]
        part = jnp.concatenate([p.astype(F32).astype(BF16) for p in parts], axis=1)
        weights += [part] * 4
    weights = jnp.concatenate(weights, axis=0)
    hi, lo = halves(got)
    zero = jnp.zeros_like(hi)
    out = []
    for r in range(4):
        mine = lane_group == r
        out.append(
            jnp.dot(jnp.where(mine, hi, zero), weights, preferred_element_type=F32)
            + jnp.dot(jnp.where(mine, lo, zero), weights, preferred_element_type=F32)
        )
    return out


def load_kernel(groups, recv_ref, req_ref, fluid_ref, out_ref):
    loads = collect([recv_ref], groups, req_ref, fluid_ref.shape[2])
    out_ref[0] = fluid_ref[0]
    for r in range(4):
        out_ref[1 + r] = fluid_ref[1 + r] - loads[r]


def join_kernel(groups, ex, ey, *refs):
    req_ref, part_ref, out_ref, xlo_ref, xhi_ref, ylo_ref, yhi_ref = refs[groups:]
    loads = collect(refs[:groups], groups, req_ref, part_ref.shape[2])
    out_ref[0] = part_ref[0]
    for r in range(4):
        out_ref[1 + r] = part_ref[1 + r] - loads[r]
    wide = ey * LANES
    for q in range(5):
        for x in range(ex - 1):
            a, b = slice(x * wide, (x + 1) * wide), slice((x + 1) * wide, (x + 2) * wide)
            total = out_ref[q, 180:216, a] + out_ref[q, 0:36, b]
            out_ref[q, 180:216, a] = total
            out_ref[q, 0:36, b] = total
        for x in range(ex):
            for y in range(ey - 1):
                base = x * wide + y * LANES
                a, b = slice(base, base + LANES), slice(base + LANES, base + 2 * LANES)
                for i in range(6):
                    total = out_ref[q, 36 * i + 30 : 36 * i + 36, a] + out_ref[q, 36 * i : 36 * i + 6, b]
                    out_ref[q, 36 * i + 30 : 36 * i + 36, a] = total
                    out_ref[q, 36 * i : 36 * i + 6, b] = total
        last = (ex - 1) * wide
        xlo_ref[q] = out_ref[q, 0:36, 0:wide]
        xhi_ref[q] = out_ref[q, 180:216, last : last + wide]
        for x in range(ex):
            dst = slice(x * LANES, (x + 1) * LANES)
            lo = slice(x * wide, x * wide + LANES)
            hi = slice((x + 1) * wide - LANES, (x + 1) * wide)
            for i in range(6):
                ylo_ref[q, 6 * i : 6 * i + 6, dst] = out_ref[q, 36 * i : 36 * i + 6, lo]
                yhi_ref[q, 6 * i : 6 * i + 6, dst] = out_ref[q, 36 * i + 30 : 36 * i + 36, hi]


def edge_kernel(ey, xl_ref, xr_ref, lo_ref, hi_ref):
    last = (ey - 1) * LANES
    for x, ref in enumerate((xl_ref, xr_ref)):
        lo_ref[x] = ref[:, 0:6, 0:LANES]
        hi_ref[x] = ref[:, 30:36, last : last + LANES]


def finish_kernel(ex, ey, part_ref, xl_ref, xr_ref, yl_ref, yr_ref, el_ref, er_ref, out_ref, work):
    for q in range(5):
        for at in range(ex * ey):
            work[at] = part_ref[q, :, at * LANES : (at + 1) * LANES]
        for y in range(ey):
            lanes = slice(y * LANES, (y + 1) * LANES)
            work[y, 0:36, :] += xl_ref[q, :, lanes]
            work[(ex - 1) * ey + y, 180:216, :] += xr_ref[q, :, lanes]
        for x in range(ex):
            lanes = slice(x * LANES, (x + 1) * LANES)
            for i in range(6):
                work[x * ey, 36 * i : 36 * i + 6, :] += yl_ref[q, 6 * i : 6 * i + 6, lanes]
                work[x * ey + ey - 1, 36 * i + 30 : 36 * i + 36, :] += yr_ref[q, 6 * i : 6 * i + 6, lanes]
        for x in range(2):
            start, at = 180 * x, x * (ex - 1) * ey
            work[at, start : start + 6, :] += el_ref[x, q]
            work[at + ey - 1, start + 30 : start + 36, :] += er_ref[x, q]
        for x in range(ex):
            for y in range(ey):
                at = x * ey + y
                lower = work[at, pl.ds(0, 36, stride=6), :]
                upper = work[at, pl.ds(5, 36, stride=6), :]
                work[at, pl.ds(5, 36, stride=6), :] = upper + pltpu.roll(lower, LANES - 1, 1)
                work[at, pl.ds(0, 36, stride=6), :] = lower + pltpu.roll(upper, 1, 1)
                out_ref[pl.ds((x * 5 + q) * NODES * ey + y, NODES, stride=ey), :] = work[at]


def call(kernel, out_shape, scratch=(), smem=0, late=0, flops=0, operands=()):
    spaces = [pltpu.SMEM if at < smem else pltpu.VMEM for at in range(len(operands))]
    if late:
        spaces[late] = pl.ANY
    return pl.pallas_call(
        kernel,
        out_shape=out_shape,
        in_specs=[pl.BlockSpec(memory_space=space) for space in spaces],
        out_specs=jax.tree.map(lambda s: pl.BlockSpec(memory_space=pltpu.VMEM), out_shape),
        scratch_shapes=list(scratch),
        cost_estimate=pl.CostEstimate(
            flops=flops, bytes_accessed=sum(x.size * 4 for x in operands), transcendentals=0
        ),
        compiler_params=pltpu.CompilerParams(vmem_limit_bytes=16 << 20),
    )(*operands)


def shape(*dims, dtype=F32):
    return jax.ShapeDtypeStruct(dims, dtype)


def step(rho, flow, hot, parent, count, basis, speed, breadth, heat):
    ex, ey, height = rho.shape[0], rho.shape[1], rho.shape[-1]
    elems = ex * ey * height
    groups, spans = lax.axis_size("gx"), lax.axis_size("gy")
    bins = parent.shape[0]
    half = bins // CHUNKS
    cap = bins // 4 // CHUNKS
    slots_t = basis.shape[-1]
    rows = -(-5 * NODES // 32) * 8
    me = lax.axis_index("gx").astype(I32).reshape(1)

    own = parent.reshape(1, bins)
    firsts = jnp.sum(
        (own // elems < jnp.arange(groups + 1, dtype=I32)[:, None]).astype(I32), axis=1
    )

    def turn(x, by):
        return lax.ppermute(x, "gx", [(i, (i + by) % groups) for i in range(groups)])

    def spread(blocks, sign):
        return [blocks[0]] + [turn(blocks[s], sign * s) for s in range(1, groups)]

    def exchange(x):
        return lax.all_to_all(x, "gx", 0, 0, tiled=True)

    ids = exchange(jnp.broadcast_to(own, (groups, bins)))
    rho_v = rho.transpose(0, 2, 3, 4, 1, 5).reshape(-1, height)
    flow_v = flow.transpose(0, 2, 3, 4, 5, 1, 6).reshape(-1, height)
    hot_v = hot.transpose(0, 2, 3, 4, 1, 5).reshape(-1, height)
    basis_v = basis.transpose(1, 2, 0, 3).reshape(18, bins, slots_t)
    speed_v = speed.transpose(1, 0, 2)

    def turn_y(x, by):
        return lax.ppermute(x, "gy", [(i, (i + by) % spans) for i in range(spans)])

    high, low = call(
        functools.partial(split_kernel, ex, ey),
        [shape(5 * NODES, elems, dtype=BF16)] * 2,
        flops=10_000_000,
        operands=(rho_v, flow_v, hot_v),
    )
    arranged = call(
        functools.partial(arrange_kernel, elems, groups),
        [shape(23, slots_t, half)] * CHUNKS + [shape(8, half, dtype=I32)] * CHUNKS,
        flops=10_000_000,
        operands=(own, count.reshape(1, bins), basis_v, speed_v, breadth, heat),
    )
    data, live = arranged[:CHUNKS], arranged[CHUNKS:]
    states, wanted = [], []
    for c in range(CHUNKS):
        blocks = [shape(groups, rows, 4 * cap)] if c == 0 else [shape(rows, 4 * cap)] * groups
        *wire, req = call(
            functools.partial(gather_kernel, c, elems, groups),
            blocks + [shape(groups * cap, LANES, dtype=I32)],
            [pltpu.VMEM((4 * rows, groups * cap), F32)],
            smem=1,
            late=4,
            flops=10_000_000,
            operands=(me, ids, high, low, ids if c == 0 else wanted[0]),
        )
        states.append([exchange(wire[0])] if c == 0 else spread(wire, 1))
        wanted.append(req)
    fluid = call(
        functools.partial(fluid_kernel, ex, ey),
        shape(5, NODES, elems),
        [
            pltpu.VMEM((5, NODES, elems), F32),
            pltpu.VMEM((3, NODES, elems), F32),
            pltpu.VMEM((NODES, elems), F32),
        ],
        flops=10_000_000,
        operands=(jnp.asarray(gll_operator()), rho_v, flow_v, hot_v),
    )
    given = []
    after = fluid
    for c in range(CHUNKS):
        wire = call(
            functools.partial(particle_kernel, c, groups),
            [shape(groups, NODES, 4 * cap)] if c == 0 else [shape(NODES, 4 * cap)] * groups,
            [
                pltpu.VMEM((4 * rows, half), F32),
                pltpu.VMEM((4 * NODES, half), F32),
                pltpu.VMEM((4, slots_t, half), F32),
            ],
            smem=2,
            late=4,
            flops=20_000_000,
            operands=(me, firsts, data[c], live[c], after, *states[c]),
        )
        after = wire[0]
        given.append([exchange(wire[0])] if c == 0 else spread(wire, -1))
    part = call(
        functools.partial(load_kernel, groups),
        shape(5, NODES, elems),
        flops=5_000_000,
        operands=(given[0][0], wanted[0], fluid),
    )
    part, xlo, xhi, ylo, yhi = call(
        functools.partial(join_kernel, groups, ex, ey),
        (
            shape(5, NODES, elems),
            shape(5, 36, ey * height),
            shape(5, 36, ey * height),
            shape(5, 36, ex * height),
            shape(5, 36, ex * height),
        ),
        flops=5_000_000,
        operands=(*given[1], wanted[1], part),
    )
    xl = lax.ppermute(xhi, "gx", [(i, i + 1) for i in range(groups - 1)])
    xr = lax.ppermute(xlo, "gx", [(i + 1, i) for i in range(groups - 1)])
    yl, yr = turn_y(yhi, 1), turn_y(ylo, -1)
    elo, ehi = call(
        functools.partial(edge_kernel, ey), [shape(2, 5, 6, height)] * 2, flops=1_000_000, operands=(xl, xr)
    )
    el, er = turn_y(ehi, 1), turn_y(elo, -1)
    out = call(
        functools.partial(finish_kernel, ex, ey),
        shape(ex * 5 * NODES * ey, height),
        [pltpu.VMEM((ex * ey, NODES, height), F32)],
        flops=5_000_000,
        operands=(part, xl, xr, yl, yr, el, er),
    )
    out = out.reshape(ex, 5, 6, 6, 6, ey, height)
    return out.transpose(0, 5, 1, 2, 3, 4, 6)


def solution(mesh):
    placed = (
        P("gx", "gy", None, None, None, None),
        P("gx", "gy", None, None, None, None, None),
        P("gx", "gy", None, None, None, None),
        P(("gx", "gy")),
        P(("gx", "gy")),
        P(("gx", "gy"), None, None, None),
        P(("gx", "gy"), None, None),
        P(("gx", "gy"), None),
        P(("gx", "gy"), None),
    )
    return jax.shard_map(
        step,
        mesh=mesh,
        in_specs=placed,
        out_specs=P("gx", "gy", None, None, None, None, None),
        check_vma=False,
    )
```

```python
import functools
import math

import jax
import jax.numpy as jnp
import numpy as np
from jax import lax
from jax.experimental import pallas as pl
from jax.experimental.pallas import tpu as pltpu
from jax.sharding import PartitionSpec as P


SPECIFIC_CP = 2.5
MU_GAS = 0.2
CONDUCTANCE = 0.2
PRANDTL = 0.72

NODES = 216
LANES = 128
CHUNKS = 2
WHOLE = (True, False)
F32 = jnp.float32
BF16 = jnp.bfloat16
I32 = jnp.int32
NT = (((1,), (1,)), ((), ()))


def gll_operator():
    root_seven = math.sqrt(7.0)
    outer_node = math.sqrt(1.0 / 3.0 + 2.0 * root_seven / 21.0)
    inner_node = math.sqrt(1.0 / 3.0 - 2.0 * root_seven / 21.0)
    points = np.array([-1.0, -outer_node, -inner_node, inner_node, outer_node, 1.0])
    outer_weight = (14.0 - root_seven) / 30.0
    inner_weight = (14.0 + root_seven) / 30.0
    w = np.array([1.0 / 15.0, outer_weight, inner_weight, inner_weight, outer_weight, 1.0 / 15.0])
    bary = np.ones(6)
    for r in range(6):
        for c in range(6):
            if c != r:
                bary[r] = bary[r] / (points[r] - points[c])
    dm = np.zeros((6, 6))
    for r in range(6):
        for c in range(6):
            if c != r:
                dm[r, c] = bary[c] / bary[r] / (points[r] - points[c])
        dm[r, r] = -np.sum(dm[r])
    eye = np.eye(6)
    volume = np.kron(np.kron(w, w), w)
    blocks = [
        np.kron(np.kron(dm, eye), eye),
        np.kron(np.kron(eye, dm), eye),
        np.kron(np.kron(eye, eye), dm),
    ]
    return (-volume[:, None] * np.concatenate(blocks, axis=1)).astype(np.float32)


def halves(x):
    hi = x.astype(BF16)
    return hi, (x - hi.astype(F32)).astype(BF16)


def thirds(x):
    hi = x.astype(BF16)
    rest = x - hi.astype(F32)
    mid = rest.astype(BF16)
    return hi, mid, (rest - mid.astype(F32)).astype(BF16)


def iota(shape, dim):
    return lax.broadcasted_iota(I32, shape, dim)


def sorted_places(ids, elems, groups):
    rows, bins = ids.shape
    shift = elems.bit_length() - 1
    assert elems == 1 << shift
    slab = jnp.right_shift(ids, shift)
    upper = (iota((bins, bins), 0) < iota((bins, bins), 1)).astype(F32).astype(BF16)
    places, firsts = [], []
    group_of = iota((groups, bins), 0)
    for d in range(rows):
        mine = jnp.broadcast_to(slab[d : d + 1], (groups, bins))
        hit = (mine == group_of).astype(F32)
        earlier = jnp.dot(hit.astype(BF16), upper, preferred_element_type=F32)
        first = jnp.sum((mine < group_of).astype(F32), axis=1, keepdims=True)
        places.append(jnp.sum(hit * (earlier + first), axis=0, keepdims=True).astype(I32))
        firsts.append(first.astype(I32))
    return places, slab, firsts


def state_columns(rho_ref, vel_ref, hot_ref, ex, ey):
    out = []
    for q in range(5):
        cols = []
        for x in range(ex):
            for y in range(ey):
                if q == 0 or q == 4:
                    ref, base = (rho_ref if q == 0 else hot_ref), x * NODES * ey + y
                else:
                    ref, base = vel_ref, (x * 3 + q - 1) * NODES * ey + y
                cols.append(ref[pl.ds(base, NODES, stride=ey), :])
        out.append(cols)
    return out


def fetch(pairs, sems):
    copies = [pltpu.make_async_copy(a, b, sems.at[n]) for n, (a, b) in enumerate(pairs)]
    for copy in copies:
        copy.start()
    for copy in copies:
        copy.wait()


def split_kernel(ex, ey, rho_in, vel_in, hot_in, hi_ref, lo_ref, rho_ref, vel_ref, hot_ref, sems):
    fetch(((rho_in, rho_ref), (vel_in, vel_ref), (hot_in, hot_ref)), sems)
    state = state_columns(rho_ref, vel_ref, hot_ref, ex, ey)
    for q in range(5):
        hi, lo = halves(jnp.concatenate(state[q], axis=1))
        hi_ref[q * NODES : (q + 1) * NODES, :] = hi
        lo_ref[q * NODES : (q + 1) * NODES, :] = lo


def block_device(c, s, me):
    return s if WHOLE[c] else jnp.bitwise_xor(me, s)


def block_view(refs, s):
    return refs[0].at[s] if len(refs) == 1 else refs[s]


def gather_kernel(c, elems, groups, me_ref, ids_ref, hi_ref, lo_ref, after_ref, *refs):
    out_refs, (req_ref, work) = refs[:-2], refs[-2:]
    bins = ids_ref.shape[1]
    me = me_ref[0]
    rows = out_refs[0].shape[-2]
    cap = LANES // 4
    slots = groups * cap
    ids = jnp.concatenate(
        [ids_ref[pl.ds(block_device(c, s, me), 1), :] for s in range(groups)], axis=0
    )
    places, slab, firsts = sorted_places(ids, elems, groups)
    elem = jnp.bitwise_and(ids, elems - 1)
    sub = iota((LANES, bins), 0)
    slot_of = iota((slots, bins), 0)
    row_table = jnp.zeros((LANES, slots), F32)
    col_table = jnp.zeros((slots, LANES), F32)
    for d in range(groups):
        place = places[d]
        first = jnp.sum(
            jnp.where(iota((groups, 1), 0) == me, firsts[d], 0).astype(F32), axis=0, keepdims=True
        ).astype(I32)
        begin = jnp.right_shift(first - c + 1, 1)
        here = (slab[d : d + 1] == me) & (jnp.bitwise_and(place, 1) == c)
        slot = jnp.where(here, jnp.right_shift(place, 1) - begin + d * cap, -1)
        match = (jnp.broadcast_to(slot, (slots, bins)) == slot_of).astype(F32).astype(BF16)
        e = jnp.broadcast_to(elem[d : d + 1], (LANES, bins))
        parts = jnp.where(
            sub == 0,
            jnp.bitwise_and(e, 255),
            jnp.where(sub == 1, jnp.right_shift(e, 8), jnp.where(sub == 2, 1, 0)),
        )
        parts = parts.astype(F32).astype(BF16)
        row_table += lax.dot_general(parts, match, NT, preferred_element_type=F32)
        col_table += lax.dot_general(match, parts, NT, preferred_element_type=F32)
    wanted = jnp.where(row_table[2:3] > 0.5, row_table[0:1] + 256.0 * row_table[1:2], -1.0).astype(I32)
    wanted_col = jnp.where(
        col_table[:, 2:3] > 0.5, col_table[:, 0:1] + 256.0 * col_table[:, 1:2], -1.0
    ).astype(I32)
    req_ref[...] = jnp.broadcast_to(wanted_col, (slots, LANES))
    onehot = (jnp.broadcast_to(wanted, (elems, slots)) == iota((elems, slots), 0)).astype(F32).astype(BF16)
    work[0 : 5 * NODES, :] = jnp.dot(
        hi_ref[...], onehot, preferred_element_type=F32
    ) + jnp.dot(lo_ref[...], onehot, preferred_element_type=F32)
    pad = 4 * rows - 5 * NODES
    work[5 * NODES : 4 * rows, :] = jnp.zeros((pad, slots), F32)
    lane_group = iota((rows, LANES), 1) // cap
    for tile in range(slots // LANES):
        block = [
            work[g * rows : (g + 1) * rows, tile * LANES : (tile + 1) * LANES] for g in range(4)
        ]
        for at in range(4):
            total = None
            for g in range(4):
                turn = ((g - at) % 4) * cap
                moved = block[g] if turn == 0 else pltpu.roll(block[g], turn, 1)
                total = moved if total is None else jnp.where(lane_group == g, moved, total)
            block_view(out_refs, tile * 4 + at)[...] = total


def arrange_kernel(elems, groups, ids_ref, count_ref, basis_ref, vel_ref, breadth_ref, hot_ref, *out_refs):
    bins = ids_ref.shape[1]
    half = bins // CHUNKS
    places, _, _ = sorted_places(ids_ref[...], elems, groups)
    place = places[0]
    target = jnp.bitwise_and(place, 1) * half + jnp.right_shift(place, 1)
    move = (jnp.broadcast_to(target, (bins, bins)) == iota((bins, bins), 0)).astype(F32).astype(BF16)
    count = jnp.broadcast_to(count_ref[...], (8, bins)).astype(F32).astype(BF16)
    live = lax.dot_general(count, move, NT, preferred_element_type=F32)
    for c in range(CHUNKS):
        out_refs[CHUNKS + c][...] = live[:, c * half : (c + 1) * half].astype(I32)
    sources = [basis_ref.at[m] for m in range(18)] + [vel_ref.at[m] for m in range(3)]
    sources += [breadth_ref, hot_ref]
    for m, source in enumerate(sources):
        hi, mid, lo = thirds(source[...])
        moved = (
            jnp.dot(move, hi, preferred_element_type=F32)
            + jnp.dot(move, mid, preferred_element_type=F32)
            + jnp.dot(move, lo, preferred_element_type=F32)
        )
        for c in range(CHUNKS):
            out_refs[c][m] = moved[c * half : (c + 1) * half].T


def fluid_kernel(ex, ey, op_ref, rho_ref, vel_ref, hot_ref, out_ref, lead, flow, push):
    state = state_columns(rho_ref, vel_ref, hot_ref, ex, ey)
    for at in range(ex * ey):
        lanes = slice(at * LANES, (at + 1) * LANES)
        rho, hot = state[0][at], state[4][at]
        u = [state[1 + d][at] for d in range(3)]
        p = rho * hot
        energy = rho * (SPECIFIC_CP * hot + 0.5 * (u[0] * u[0] + u[1] * u[1] + u[2] * u[2]))
        push[:, lanes] = p
        lead[0, :, lanes] = rho
        lead[4, :, lanes] = energy + p
        for d in range(3):
            flow[d, :, lanes] = u[d]
            lead[1 + d, :, lanes] = rho * u[d]

    def component(q, _):
        parts = []
        for d in range(3):
            extra = jnp.where(q == d + 1, 1.0, 0.0).astype(F32)
            parts.append(lead[q] * flow[d] + extra * push[...])
        flux = jnp.concatenate(parts, axis=0)
        out_ref[q] = jnp.dot(
            op_ref[...], flux, preferred_element_type=F32, precision=lax.Precision.HIGHEST
        )
        return 0

    lax.fori_loop(0, 5, component, 0)


def particle_kernel(c, groups, me_ref, firsts_ref, data_ref, live_ref, after_ref, *refs):
    host, work, force = refs[-3:]
    blocks = 1 if WHOLE[c] else groups
    recv_refs, out_refs = refs[:blocks], refs[blocks:-3]
    rows = recv_refs[0].shape[-2]
    cap = LANES // 4
    me = me_ref[0]
    slots_t = data_ref.shape[1]
    width = data_ref.shape[2]
    begins, ends = [], []
    for s in range(groups):
        g = block_device(c, s, me)
        begins.append(jnp.right_shift(firsts_ref[g] - c + 1, 1))
        ends.append(jnp.right_shift(firsts_ref[g + 1] - c + 1, 1))

    row = iota((LANES, width), 0)
    col = iota((LANES, width), 1)
    slot = jnp.bitwise_and(row, cap - 1)
    lane_group = jnp.right_shift(row, cap.bit_length() - 1)
    bases = [(col - slot == begins[d]) & (col < ends[d]) for d in range(groups)]
    got_hi, got_lo = halves(jnp.concatenate([block_view(recv_refs, s)[...] for s in range(groups)], axis=1))
    for g in range(4):
        weights = jnp.concatenate(
            [(bases[d] & (lane_group == g)).astype(F32).astype(BF16) for d in range(groups)], axis=0
        )
        host[g * rows : (g + 1) * rows, :] = jnp.dot(
            got_hi, weights, preferred_element_type=F32
        ) + jnp.dot(got_lo, weights, preferred_element_type=F32)

    step = 16
    live = live_ref[0:1, :]

    def sample(tb, _):
        at = pl.ds(pl.multiple_of(tb * step, step), step)
        b0 = [data_ref[i, at, :] for i in range(6)]
        b1 = [data_ref[6 + i, at, :] for i in range(6)]
        b2 = [data_ref[12 + i, at, :] for i in range(6)]
        sampled = []
        for q in range(5):
            over_i = None
            for i in range(6):
                over_j = None
                for j in range(6):
                    over_k = None
                    for k in range(6):
                        n = q * NODES + i * 36 + j * 6 + k
                        term = host[n : n + 1, :] * b2[k]
                        over_k = term if over_k is None else over_k + term
                    term = over_k * b1[j]
                    over_j = term if over_j is None else over_j + term
                term = over_j * b0[i]
                over_i = term if over_i is None else over_i + term
            sampled.append(over_i)
        v = [data_ref[18 + d, at, :] for d in range(3)]
        breadth, hot = data_ref[21, at, :], data_ref[22, at, :]
        rel = [sampled[1 + d] - v[d] for d in range(3)]
        ratio = sampled[0] * breadth * (1.0 / MU_GAS)
        reynolds = ratio * ratio * (rel[0] * rel[0] + rel[1] * rel[1] + rel[2] * rel[2]) + 1.0
        drag = (3.0 * math.pi * MU_GAS) * (breadth * (1.0 + 0.15 * jnp.exp(0.3435 * jnp.log(reynolds))))
        transfer = 2.0 + 0.6 * PRANDTL ** (1.0 / 3.0) * jnp.sqrt(jnp.sqrt(reynolds))
        heat = (math.pi * CONDUCTANCE) * breadth * transfer * (sampled[4] - hot)
        on = iota((step, width), 0) + tb * step < live
        pull = [drag * rel[d] for d in range(3)]
        power = pull[0] * v[0] + pull[1] * v[1] + pull[2] * v[2] + heat
        for r, value in enumerate(pull + [power]):
            force[r, at, :] = jnp.where(on, value, 0.0)
        return 0

    lax.fori_loop(0, slots_t // step, sample, 0)

    def project(ij, _):
        i, j = ij // 6, ij % 6
        acc = [[None] * 6 for _ in range(4)]
        for tb in range(slots_t // 8):
            at = slice(tb * 8, tb * 8 + 8)
            both = data_ref[i, at, :] * data_ref[6 + j, at, :]
            b2 = [data_ref[12 + k, at, :] for k in range(6)]
            for r in range(4):
                g = force[r, at, :] * both
                for k in range(6):
                    term = g * b2[k]
                    acc[r][k] = term if acc[r][k] is None else acc[r][k] + term
        for r in range(4):
            for k in range(6):
                work[pl.ds(r * NODES + ij * 6 + k, 1), :] = jnp.sum(acc[r][k], axis=0, keepdims=True)
        return 0

    lax.fori_loop(0, 36, project, 0)

    row = iota((width, LANES), 0)
    col = iota((width, LANES), 1)
    slot = jnp.bitwise_and(col, cap - 1)
    lane_group = jnp.right_shift(col, cap.bit_length() - 1)
    give_hi, give_lo = halves(
        jnp.concatenate([work[r * NODES : (r + 1) * NODES, :] for r in range(4)], axis=1)
    )
    for d in range(groups):
        base = (row - slot == begins[d]) & (row < ends[d])
        weights = jnp.concatenate(
            [(base & (lane_group == r)).astype(F32).astype(BF16) for r in range(4)], axis=0
        )
        block_view(out_refs, d)[...] = jnp.dot(give_hi, weights, preferred_element_type=F32) + jnp.dot(
            give_lo, weights, preferred_element_type=F32
        )


def collect(recv_refs, groups, req_ref, elems):
    cap = LANES // 4
    got = jnp.concatenate([block_view(recv_refs, s)[...] for s in range(groups)], axis=1)
    lane_group = jnp.right_shift(jnp.bitwise_and(iota(got.shape, 1), LANES - 1), cap.bit_length() - 1)
    weights = []
    for d in range(groups):
        want = req_ref[d * cap : (d + 1) * cap, :]
        parts = [(want == iota(want.shape, 1) + t * LANES) for t in range(elems // LANES)]
        part = jnp.concatenate([p.astype(F32).astype(BF16) for p in parts], axis=1)
        weights += [part] * 4
    weights = jnp.concatenate(weights, axis=0)
    hi, lo = halves(got)
    zero = jnp.zeros_like(hi)
    out = []
    for r in range(4):
        mine = lane_group == r
        out.append(
            jnp.dot(jnp.where(mine, hi, zero), weights, preferred_element_type=F32)
            + jnp.dot(jnp.where(mine, lo, zero), weights, preferred_element_type=F32)
        )
    return out


def load_kernel(groups, *refs):
    req_ref, fluid_ref, out_ref = refs[-3:]
    loads = collect(refs[:-3], groups, req_ref, fluid_ref.shape[2])
    out_ref[0] = fluid_ref[0]
    for r in range(4):
        out_ref[1 + r] = fluid_ref[1 + r] - loads[r]


def join_kernel(groups, ex, ey, *refs):
    req_ref, part_ref, out_ref, xlo_ref, xhi_ref, ylo_ref, yhi_ref = refs[-7:]
    loads = collect(refs[:-7], groups, req_ref, part_ref.shape[2])
    out_ref[0] = part_ref[0]
    for r in range(4):
        out_ref[1 + r] = part_ref[1 + r] - loads[r]
    wide = ey * LANES
    for q in range(5):
        for x in range(ex - 1):
            a, b = slice(x * wide, (x + 1) * wide), slice((x + 1) * wide, (x + 2) * wide)
            total = out_ref[q, 180:216, a] + out_ref[q, 0:36, b]
            out_ref[q, 180:216, a] = total
            out_ref[q, 0:36, b] = total
        for x in range(ex):
            for y in range(ey - 1):
                base = x * wide + y * LANES
                a, b = slice(base, base + LANES), slice(base + LANES, base + 2 * LANES)
                for i in range(6):
                    total = out_ref[q, 36 * i + 30 : 36 * i + 36, a] + out_ref[q, 36 * i : 36 * i + 6, b]
                    out_ref[q, 36 * i + 30 : 36 * i + 36, a] = total
                    out_ref[q, 36 * i : 36 * i + 6, b] = total
        last = (ex - 1) * wide
        xlo_ref[q] = out_ref[q, 0:36, 0:wide]
        xhi_ref[q] = out_ref[q, 180:216, last : last + wide]
        for x in range(ex):
            dst = slice(x * LANES, (x + 1) * LANES)
            lo = slice(x * wide, x * wide + LANES)
            hi = slice((x + 1) * wide - LANES, (x + 1) * wide)
            for i in range(6):
                ylo_ref[q, 6 * i : 6 * i + 6, dst] = out_ref[q, 36 * i : 36 * i + 6, lo]
                yhi_ref[q, 6 * i : 6 * i + 6, dst] = out_ref[q, 36 * i + 30 : 36 * i + 36, hi]


def edge_kernel(ey, xl_ref, xr_ref, lo_ref, hi_ref):
    last = (ey - 1) * LANES
    for x, ref in enumerate((xl_ref, xr_ref)):
        lo_ref[x] = ref[:, 0:6, 0:LANES]
        hi_ref[x] = ref[:, 30:36, last : last + LANES]


def finish_kernel(ex, ey, part_ref, xl_ref, xr_ref, yl_ref, yr_ref, el_ref, er_ref, out_ref, work):
    for q in range(5):
        for at in range(ex * ey):
            work[at] = part_ref[q, :, at * LANES : (at + 1) * LANES]
        for y in range(ey):
            lanes = slice(y * LANES, (y + 1) * LANES)
            work[y, 0:36, :] += xl_ref[q, :, lanes]
            work[(ex - 1) * ey + y, 180:216, :] += xr_ref[q, :, lanes]
        for x in range(ex):
            lanes = slice(x * LANES, (x + 1) * LANES)
            for i in range(6):
                work[x * ey, 36 * i : 36 * i + 6, :] += yl_ref[q, 6 * i : 6 * i + 6, lanes]
                work[x * ey + ey - 1, 36 * i + 30 : 36 * i + 36, :] += yr_ref[q, 6 * i : 6 * i + 6, lanes]
        for x in range(2):
            start, at = 180 * x, x * (ex - 1) * ey
            work[at, start : start + 6, :] += el_ref[x, q]
            work[at + ey - 1, start + 30 : start + 36, :] += er_ref[x, q]
        for x in range(ex):
            for y in range(ey):
                at = x * ey + y
                lower = work[at, pl.ds(0, 36, stride=6), :]
                upper = work[at, pl.ds(5, 36, stride=6), :]
                work[at, pl.ds(5, 36, stride=6), :] = upper + pltpu.roll(lower, LANES - 1, 1)
                work[at, pl.ds(0, 36, stride=6), :] = lower + pltpu.roll(upper, 1, 1)
                out_ref[pl.ds((x * 5 + q) * NODES * ey + y, NODES, stride=ey), :] = work[at]


def call(kernel, out_shape, scratch=(), smem=0, late=0, hbm=(), flops=0, operands=()):
    spaces = [pltpu.SMEM if at < smem else pltpu.VMEM for at in range(len(operands))]
    if late:
        spaces[late] = pl.ANY
    for at in hbm:
        spaces[at] = pltpu.HBM
    return pl.pallas_call(
        kernel,
        out_shape=out_shape,
        in_specs=[pl.BlockSpec(memory_space=space) for space in spaces],
        out_specs=jax.tree.map(lambda s: pl.BlockSpec(memory_space=pltpu.VMEM), out_shape),
        scratch_shapes=list(scratch),
        cost_estimate=pl.CostEstimate(
            flops=flops, bytes_accessed=sum(x.size * 4 for x in operands), transcendentals=0
        ),
        compiler_params=pltpu.CompilerParams(vmem_limit_bytes=16 << 20),
    )(*operands)


def shape(*dims, dtype=F32):
    return jax.ShapeDtypeStruct(dims, dtype)


def step(rho, flow, hot, parent, count, basis, speed, breadth, heat):
    ex, ey, height = rho.shape[0], rho.shape[1], rho.shape[-1]
    elems = ex * ey * height
    groups, spans = lax.axis_size("gx"), lax.axis_size("gy")
    bins = parent.shape[0]
    half = bins // CHUNKS
    cap = bins // 4 // CHUNKS
    slots_t = basis.shape[-1]
    rows = -(-5 * NODES // 32) * 8
    me = lax.axis_index("gx").astype(I32).reshape(1)

    own = parent.reshape(1, bins)
    firsts = jnp.sum(
        (own // elems < jnp.arange(groups + 1, dtype=I32)[:, None]).astype(I32), axis=1
    )

    def swap(x, by):
        return lax.ppermute(x, "gx", [(i, i ^ by) for i in range(groups)])

    def exchange(x):
        return lax.all_to_all(x, "gx", 0, 0, tiled=True)

    def send(c, blocks):
        if WHOLE[c]:
            return [exchange(blocks[0])]
        got = {s: swap(blocks[s], s) for s in range(groups - 1, 0, -1)}
        return [blocks[0]] + [got[s] for s in range(1, groups)]

    ids = exchange(jnp.broadcast_to(own, (groups, bins)))
    rho_v = rho.transpose(0, 2, 3, 4, 1, 5).reshape(-1, height)
    flow_v = flow.transpose(0, 2, 3, 4, 5, 1, 6).reshape(-1, height)
    hot_v = hot.transpose(0, 2, 3, 4, 1, 5).reshape(-1, height)
    basis_v = basis.transpose(1, 2, 0, 3).reshape(18, bins, slots_t)
    speed_v = speed.transpose(1, 0, 2)

    def turn_y(x, by):
        return lax.ppermute(x, "gy", [(i, (i + by) % spans) for i in range(spans)])

    high, low = call(
        functools.partial(split_kernel, ex, ey),
        [shape(5 * NODES, elems, dtype=BF16)] * 2,
        [pltpu.VMEM(x.shape, F32) for x in (rho_v, flow_v, hot_v)] + [pltpu.SemaphoreType.DMA((3,))],
        hbm=(0, 1, 2),
        flops=10_000_000,
        operands=(rho_v, flow_v, hot_v),
    )
    arranged = call(
        functools.partial(arrange_kernel, elems, groups),
        [shape(23, slots_t, half)] * CHUNKS + [shape(8, half, dtype=I32)] * CHUNKS,
        flops=10_000_000,
        operands=(own, count.reshape(1, bins), basis_v, speed_v, breadth, heat),
    )
    data, live = arranged[:CHUNKS], arranged[CHUNKS:]
    states, wanted = [], []
    for c in range(CHUNKS):
        blocks = [shape(groups, rows, 4 * cap)] if WHOLE[c] else [shape(rows, 4 * cap)] * groups
        *wire, req = call(
            functools.partial(gather_kernel, c, elems, groups),
            blocks + [shape(groups * cap, LANES, dtype=I32)],
            [pltpu.VMEM((4 * rows, groups * cap), F32)],
            smem=1,
            late=4,
            flops=10_000_000,
            operands=(me, ids, high, low, ids if c == 0 else wanted[0]),
        )
        states.append(send(c, wire))
        wanted.append(req)
    fluid = call(
        functools.partial(fluid_kernel, ex, ey),
        shape(5, NODES, elems),
        [
            pltpu.VMEM((5, NODES, elems), F32),
            pltpu.VMEM((3, NODES, elems), F32),
            pltpu.VMEM((NODES, elems), F32),
        ],
        flops=10_000_000,
        operands=(jnp.asarray(gll_operator()), rho_v, flow_v, hot_v),
    )
    given = []
    after = wanted[1]
    for c in range(CHUNKS):
        wire = call(
            functools.partial(particle_kernel, c, groups),
            [shape(groups, NODES, 4 * cap)] if WHOLE[c] else [shape(NODES, 4 * cap)] * groups,
            [
                pltpu.VMEM((4 * rows, half), F32),
                pltpu.VMEM((4 * NODES, half), F32),
                pltpu.VMEM((4, slots_t, half), F32),
            ],
            smem=2,
            late=4,
            flops=20_000_000,
            operands=(me, firsts, data[c], live[c], after, *states[c]),
        )
        after = wire[0]
        given.append(send(c, wire))
    part = call(
        functools.partial(load_kernel, groups),
        shape(5, NODES, elems),
        flops=5_000_000,
        operands=(*given[0], wanted[0], fluid),
    )
    part, xlo, xhi, ylo, yhi = call(
        functools.partial(join_kernel, groups, ex, ey),
        (
            shape(5, NODES, elems),
            shape(5, 36, ey * height),
            shape(5, 36, ey * height),
            shape(5, 36, ex * height),
            shape(5, 36, ex * height),
        ),
        flops=5_000_000,
        operands=(*given[1], wanted[1], part),
    )
    xl = lax.ppermute(xhi, "gx", [(i, i + 1) for i in range(groups - 1)])
    xr = lax.ppermute(xlo, "gx", [(i + 1, i) for i in range(groups - 1)])
    yl, yr = turn_y(yhi, 1), turn_y(ylo, -1)
    elo, ehi = call(
        functools.partial(edge_kernel, ey), [shape(2, 5, 6, height)] * 2, flops=1_000_000, operands=(xl, xr)
    )
    el, er = turn_y(ehi, 1), turn_y(elo, -1)
    out = call(
        functools.partial(finish_kernel, ex, ey),
        shape(ex * 5 * NODES * ey, height),
        [pltpu.VMEM((ex * ey, NODES, height), F32)],
        flops=5_000_000,
        operands=(part, xl, xr, yl, yr, el, er),
    )
    out = out.reshape(ex, 5, 6, 6, 6, ey, height)
    return out.transpose(0, 5, 1, 2, 3, 4, 6)


def solution(mesh):
    placed = (
        P("gx", "gy", None, None, None, None),
        P("gx", "gy", None, None, None, None, None),
        P("gx", "gy", None, None, None, None),
        P(("gx", "gy")),
        P(("gx", "gy")),
        P(("gx", "gy"), None, None, None),
        P(("gx", "gy"), None, None),
        P(("gx", "gy"), None),
        P(("gx", "gy"), None),
    )
    return jax.shard_map(
        step,
        mesh=mesh,
        in_specs=placed,
        out_specs=P("gx", "gy", None, None, None, None, None),
        check_vma=False,
    )
```

```python
import functools
import math

import jax
import jax.numpy as jnp
import numpy as np
from jax import lax
from jax.experimental import pallas as pl
from jax.experimental.pallas import tpu as pltpu
from jax.sharding import PartitionSpec as P


SPECIFIC_CP = 2.5
MU_GAS = 0.2
CONDUCTANCE = 0.2
PRANDTL = 0.72

NODES = 216
LANES = 128
CHUNKS = 2
WHOLE = (True, False)
F32 = jnp.float32
BF16 = jnp.bfloat16
I32 = jnp.int32
NT = (((1,), (1,)), ((), ()))


def gll_operator():
    root_seven = math.sqrt(7.0)
    outer_node = math.sqrt(1.0 / 3.0 + 2.0 * root_seven / 21.0)
    inner_node = math.sqrt(1.0 / 3.0 - 2.0 * root_seven / 21.0)
    points = np.array([-1.0, -outer_node, -inner_node, inner_node, outer_node, 1.0])
    outer_weight = (14.0 - root_seven) / 30.0
    inner_weight = (14.0 + root_seven) / 30.0
    w = np.array([1.0 / 15.0, outer_weight, inner_weight, inner_weight, outer_weight, 1.0 / 15.0])
    bary = np.ones(6)
    for r in range(6):
        for c in range(6):
            if c != r:
                bary[r] = bary[r] / (points[r] - points[c])
    dm = np.zeros((6, 6))
    for r in range(6):
        for c in range(6):
            if c != r:
                dm[r, c] = bary[c] / bary[r] / (points[r] - points[c])
        dm[r, r] = -np.sum(dm[r])
    eye = np.eye(6)
    volume = np.kron(np.kron(w, w), w)
    blocks = [
        np.kron(np.kron(dm, eye), eye),
        np.kron(np.kron(eye, dm), eye),
        np.kron(np.kron(eye, eye), dm),
    ]
    return (-volume[:, None] * np.concatenate(blocks, axis=1)).astype(np.float32)


def halves(x):
    hi = x.astype(BF16)
    return hi, (x - hi.astype(F32)).astype(BF16)


def thirds(x):
    hi = x.astype(BF16)
    rest = x - hi.astype(F32)
    mid = rest.astype(BF16)
    return hi, mid, (rest - mid.astype(F32)).astype(BF16)


def iota(shape, dim):
    return lax.broadcasted_iota(I32, shape, dim)


def sorted_places(ids, elems, groups):
    rows, bins = ids.shape
    shift = elems.bit_length() - 1
    assert elems == 1 << shift
    slab = jnp.right_shift(ids, shift)
    upper = (iota((bins, bins), 0) < iota((bins, bins), 1)).astype(F32).astype(BF16)
    places, firsts = [], []
    group_of = iota((groups, bins), 0)
    for d in range(rows):
        mine = jnp.broadcast_to(slab[d : d + 1], (groups, bins))
        hit = (mine == group_of).astype(F32)
        earlier = jnp.dot(hit.astype(BF16), upper, preferred_element_type=F32)
        first = jnp.sum((mine < group_of).astype(F32), axis=1, keepdims=True)
        places.append(jnp.sum(hit * (earlier + first), axis=0, keepdims=True).astype(I32))
        firsts.append(first.astype(I32))
    return places, slab, firsts


def state_columns(rho_ref, vel_ref, hot_ref, ex, ey):
    out = []
    for q in range(5):
        cols = []
        for x in range(ex):
            for y in range(ey):
                if q == 0 or q == 4:
                    ref, base = (rho_ref if q == 0 else hot_ref), x * NODES * ey + y
                else:
                    ref, base = vel_ref, (x * 3 + q - 1) * NODES * ey + y
                cols.append(ref[pl.ds(base, NODES, stride=ey), :])
        out.append(cols)
    return out


def fetch(pairs, sems):
    copies = [pltpu.make_async_copy(a, b, sems.at[n]) for n, (a, b) in enumerate(pairs)]
    for copy in copies:
        copy.start()
    for copy in copies:
        copy.wait()


def split_kernel(ex, ey, rho_in, vel_in, hot_in, hi_ref, lo_ref, rho_ref, vel_ref, hot_ref, sems):
    fetch(((rho_in, rho_ref), (vel_in, vel_ref), (hot_in, hot_ref)), sems)
    state = state_columns(rho_ref, vel_ref, hot_ref, ex, ey)
    for q in range(5):
        hi, lo = halves(jnp.concatenate(state[q], axis=1))
        hi_ref[q * NODES : (q + 1) * NODES, :] = hi
        lo_ref[q * NODES : (q + 1) * NODES, :] = lo


def block_device(c, s, me):
    return s if WHOLE[c] else jnp.bitwise_xor(me, s)


def block_view(refs, s):
    return refs[0].at[s] if len(refs) == 1 else refs[s]


def gather_kernel(c, elems, groups, me_ref, ids_ref, hi_ref, lo_ref, after_ref, *refs):
    out_refs, (req_ref, work) = refs[:-2], refs[-2:]
    bins = ids_ref.shape[1]
    me = me_ref[0]
    rows = out_refs[0].shape[-2]
    cap = LANES // 4
    slots = groups * cap
    ids = jnp.concatenate(
        [ids_ref[pl.ds(block_device(c, s, me), 1), :] for s in range(groups)], axis=0
    )
    places, slab, firsts = sorted_places(ids, elems, groups)
    elem = jnp.bitwise_and(ids, elems - 1)
    sub = iota((LANES, bins), 0)
    slot_of = iota((slots, bins), 0)
    row_table = jnp.zeros((LANES, slots), F32)
    col_table = jnp.zeros((slots, LANES), F32)
    for d in range(groups):
        place = places[d]
        first = jnp.sum(
            jnp.where(iota((groups, 1), 0) == me, firsts[d], 0).astype(F32), axis=0, keepdims=True
        ).astype(I32)
        begin = jnp.right_shift(first - c + 1, 1)
        here = (slab[d : d + 1] == me) & (jnp.bitwise_and(place, 1) == c)
        slot = jnp.where(here, jnp.right_shift(place, 1) - begin + d * cap, -1)
        match = (jnp.broadcast_to(slot, (slots, bins)) == slot_of).astype(F32).astype(BF16)
        e = jnp.broadcast_to(elem[d : d + 1], (LANES, bins))
        parts = jnp.where(
            sub == 0,
            jnp.bitwise_and(e, 255),
            jnp.where(sub == 1, jnp.right_shift(e, 8), jnp.where(sub == 2, 1, 0)),
        )
        parts = parts.astype(F32).astype(BF16)
        row_table += lax.dot_general(parts, match, NT, preferred_element_type=F32)
        col_table += lax.dot_general(match, parts, NT, preferred_element_type=F32)
    wanted = jnp.where(row_table[2:3] > 0.5, row_table[0:1] + 256.0 * row_table[1:2], -1.0).astype(I32)
    wanted_col = jnp.where(
        col_table[:, 2:3] > 0.5, col_table[:, 0:1] + 256.0 * col_table[:, 1:2], -1.0
    ).astype(I32)
    req_ref[...] = jnp.broadcast_to(wanted_col, (slots, LANES))
    onehot = (jnp.broadcast_to(wanted, (elems, slots)) == iota((elems, slots), 0)).astype(F32).astype(BF16)
    work[0 : 5 * NODES, :] = jnp.dot(
        hi_ref[...], onehot, preferred_element_type=F32
    ) + jnp.dot(lo_ref[...], onehot, preferred_element_type=F32)
    pad = 4 * rows - 5 * NODES
    work[5 * NODES : 4 * rows, :] = jnp.zeros((pad, slots), F32)
    lane_group = iota((rows, LANES), 1) // cap
    for tile in range(slots // LANES):
        block = [
            work[g * rows : (g + 1) * rows, tile * LANES : (tile + 1) * LANES] for g in range(4)
        ]
        for at in range(4):
            total = None
            for g in range(4):
                turn = ((g - at) % 4) * cap
                moved = block[g] if turn == 0 else pltpu.roll(block[g], turn, 1)
                total = moved if total is None else jnp.where(lane_group == g, moved, total)
            block_view(out_refs, tile * 4 + at)[...] = total


def arrange_kernel(elems, groups, ids_ref, count_ref, basis_ref, vel_ref, breadth_ref, hot_ref, *out_refs):
    bins = ids_ref.shape[1]
    half = bins // CHUNKS
    places, _, _ = sorted_places(ids_ref[...], elems, groups)
    place = places[0]
    target = jnp.bitwise_and(place, 1) * half + jnp.right_shift(place, 1)
    move = (jnp.broadcast_to(target, (bins, bins)) == iota((bins, bins), 0)).astype(F32).astype(BF16)
    count = jnp.broadcast_to(count_ref[...], (8, bins)).astype(F32).astype(BF16)
    live = lax.dot_general(count, move, NT, preferred_element_type=F32)
    for c in range(CHUNKS):
        out_refs[CHUNKS + c][...] = live[:, c * half : (c + 1) * half].astype(I32)
    sources = [basis_ref.at[m] for m in range(18)] + [vel_ref.at[m] for m in range(3)]
    sources += [breadth_ref, hot_ref]
    for m, source in enumerate(sources):
        hi, mid, lo = thirds(source[...])
        moved = (
            jnp.dot(move, hi, preferred_element_type=F32)
            + jnp.dot(move, mid, preferred_element_type=F32)
            + jnp.dot(move, lo, preferred_element_type=F32)
        )
        for c in range(CHUNKS):
            out_refs[c][m] = moved[c * half : (c + 1) * half].T


def fluid_kernel(ex, ey, op_ref, rho_ref, vel_ref, hot_ref, out_ref, lead, flow, push):
    state = state_columns(rho_ref, vel_ref, hot_ref, ex, ey)
    for at in range(ex * ey):
        lanes = slice(at * LANES, (at + 1) * LANES)
        rho, hot = state[0][at], state[4][at]
        u = [state[1 + d][at] for d in range(3)]
        p = rho * hot
        energy = rho * (SPECIFIC_CP * hot + 0.5 * (u[0] * u[0] + u[1] * u[1] + u[2] * u[2]))
        push[:, lanes] = p
        lead[0, :, lanes] = rho
        lead[4, :, lanes] = energy + p
        for d in range(3):
            flow[d, :, lanes] = u[d]
            lead[1 + d, :, lanes] = rho * u[d]

    def component(q, _):
        parts = []
        for d in range(3):
            extra = jnp.where(q == d + 1, 1.0, 0.0).astype(F32)
            parts.append(lead[q] * flow[d] + extra * push[...])
        flux = jnp.concatenate(parts, axis=0)
        out_ref[q] = jnp.dot(
            op_ref[...], flux, preferred_element_type=F32, precision=lax.Precision.HIGHEST
        )
        return 0

    lax.fori_loop(0, 5, component, 0)


def particle_kernel(c, groups, me_ref, firsts_ref, data_ref, live_ref, after_ref, *refs):
    host, work, force = refs[-3:]
    blocks = 1 if WHOLE[c] else groups
    recv_refs, out_refs = refs[:blocks], refs[blocks:-3]
    rows = recv_refs[0].shape[-2]
    cap = LANES // 4
    me = me_ref[0]
    slots_t = data_ref.shape[1]
    width = data_ref.shape[2]
    begins, ends = [], []
    for s in range(groups):
        g = block_device(c, s, me)
        begins.append(jnp.right_shift(firsts_ref[g] - c + 1, 1))
        ends.append(jnp.right_shift(firsts_ref[g + 1] - c + 1, 1))

    row = iota((LANES, width), 0)
    col = iota((LANES, width), 1)
    slot = jnp.bitwise_and(row, cap - 1)
    lane_group = jnp.right_shift(row, cap.bit_length() - 1)
    bases = [(col - slot == begins[d]) & (col < ends[d]) for d in range(groups)]
    got_hi, got_lo = halves(jnp.concatenate([block_view(recv_refs, s)[...] for s in range(groups)], axis=1))
    for g in range(4):
        weights = jnp.concatenate(
            [(bases[d] & (lane_group == g)).astype(F32).astype(BF16) for d in range(groups)], axis=0
        )
        host[g * rows : (g + 1) * rows, :] = jnp.dot(
            got_hi, weights, preferred_element_type=F32
        ) + jnp.dot(got_lo, weights, preferred_element_type=F32)

    step = 16
    live = live_ref[0:1, :]

    def sample(tb, _):
        at = pl.ds(pl.multiple_of(tb * step, step), step)
        b0 = [data_ref[i, at, :] for i in range(6)]
        b1 = [data_ref[6 + i, at, :] for i in range(6)]
        b2 = [data_ref[12 + i, at, :] for i in range(6)]
        sampled = []
        for q in range(5):
            over_i = None
            for i in range(6):
                over_j = None
                for j in range(6):
                    over_k = None
                    for k in range(6):
                        n = q * NODES + i * 36 + j * 6 + k
                        term = host[n : n + 1, :] * b2[k]
                        over_k = term if over_k is None else over_k + term
                    term = over_k * b1[j]
                    over_j = term if over_j is None else over_j + term
                term = over_j * b0[i]
                over_i = term if over_i is None else over_i + term
            sampled.append(over_i)
        v = [data_ref[18 + d, at, :] for d in range(3)]
        breadth, hot = data_ref[21, at, :], data_ref[22, at, :]
        rel = [sampled[1 + d] - v[d] for d in range(3)]
        ratio = sampled[0] * breadth * (1.0 / MU_GAS)
        reynolds = ratio * ratio * (rel[0] * rel[0] + rel[1] * rel[1] + rel[2] * rel[2]) + 1.0
        drag = (3.0 * math.pi * MU_GAS) * (breadth * (1.0 + 0.15 * jnp.exp(0.3435 * jnp.log(reynolds))))
        transfer = 2.0 + 0.6 * PRANDTL ** (1.0 / 3.0) * jnp.sqrt(jnp.sqrt(reynolds))
        heat = (math.pi * CONDUCTANCE) * breadth * transfer * (sampled[4] - hot)
        on = iota((step, width), 0) + tb * step < live
        pull = [drag * rel[d] for d in range(3)]
        power = pull[0] * v[0] + pull[1] * v[1] + pull[2] * v[2] + heat
        for r, value in enumerate(pull + [power]):
            force[r, at, :] = jnp.where(on, value, 0.0)
        return 0

    lax.fori_loop(0, slots_t // step, sample, 0)

    def project(ij, _):
        i, j = ij // 6, ij % 6
        acc = [[None] * 6 for _ in range(4)]
        for tb in range(slots_t // 8):
            at = slice(tb * 8, tb * 8 + 8)
            both = data_ref[i, at, :] * data_ref[6 + j, at, :]
            b2 = [data_ref[12 + k, at, :] for k in range(6)]
            for r in range(4):
                g = force[r, at, :] * both
                for k in range(6):
                    term = g * b2[k]
                    acc[r][k] = term if acc[r][k] is None else acc[r][k] + term
        for r in range(4):
            for k in range(6):
                work[pl.ds(r * NODES + ij * 6 + k, 1), :] = jnp.sum(acc[r][k], axis=0, keepdims=True)
        return 0

    lax.fori_loop(0, 36, project, 0)

    row = iota((width, LANES), 0)
    col = iota((width, LANES), 1)
    slot = jnp.bitwise_and(col, cap - 1)
    lane_group = jnp.right_shift(col, cap.bit_length() - 1)
    give_hi, give_lo = halves(
        jnp.concatenate([work[r * NODES : (r + 1) * NODES, :] for r in range(4)], axis=1)
    )
    for d in range(groups):
        base = (row - slot == begins[d]) & (row < ends[d])
        weights = jnp.concatenate(
            [(base & (lane_group == r)).astype(F32).astype(BF16) for r in range(4)], axis=0
        )
        block_view(out_refs, d)[...] = jnp.dot(give_hi, weights, preferred_element_type=F32) + jnp.dot(
            give_lo, weights, preferred_element_type=F32
        )


def collect(recv_refs, groups, req_ref, elems):
    cap = LANES // 4
    got = jnp.concatenate([block_view(recv_refs, s)[...] for s in range(groups)], axis=1)
    lane_group = jnp.right_shift(jnp.bitwise_and(iota(got.shape, 1), LANES - 1), cap.bit_length() - 1)
    weights = []
    for d in range(groups):
        want = req_ref[d * cap : (d + 1) * cap, :]
        parts = [(want == iota(want.shape, 1) + t * LANES) for t in range(elems // LANES)]
        part = jnp.concatenate([p.astype(F32).astype(BF16) for p in parts], axis=1)
        weights += [part] * 4
    weights = jnp.concatenate(weights, axis=0)
    hi, lo = halves(got)
    zero = jnp.zeros_like(hi)
    out = []
    for r in range(4):
        mine = lane_group == r
        out.append(
            jnp.dot(jnp.where(mine, hi, zero), weights, preferred_element_type=F32)
            + jnp.dot(jnp.where(mine, lo, zero), weights, preferred_element_type=F32)
        )
    return out


def load_kernel(groups, *refs):
    req_ref, fluid_ref, out_ref = refs[-3:]
    loads = collect(refs[:-3], groups, req_ref, fluid_ref.shape[2])
    out_ref[0] = fluid_ref[0]
    for r in range(4):
        out_ref[1 + r] = fluid_ref[1 + r] - loads[r]


def join_kernel(groups, ex, ey, *refs):
    req_ref, part_ref, out_ref, xlo_ref, xhi_ref, ylo_ref, yhi_ref = refs[-7:]
    loads = collect(refs[:-7], groups, req_ref, part_ref.shape[2])
    out_ref[0] = part_ref[0]
    for r in range(4):
        out_ref[1 + r] = part_ref[1 + r] - loads[r]
    wide = ey * LANES
    for q in range(5):
        for x in range(ex - 1):
            a, b = slice(x * wide, (x + 1) * wide), slice((x + 1) * wide, (x + 2) * wide)
            total = out_ref[q, 180:216, a] + out_ref[q, 0:36, b]
            out_ref[q, 180:216, a] = total
            out_ref[q, 0:36, b] = total
        for x in range(ex):
            for y in range(ey - 1):
                base = x * wide + y * LANES
                a, b = slice(base, base + LANES), slice(base + LANES, base + 2 * LANES)
                for i in range(6):
                    total = out_ref[q, 36 * i + 30 : 36 * i + 36, a] + out_ref[q, 36 * i : 36 * i + 6, b]
                    out_ref[q, 36 * i + 30 : 36 * i + 36, a] = total
                    out_ref[q, 36 * i : 36 * i + 6, b] = total
        last = (ex - 1) * wide
        face = slice(36 * q, 36 * q + 36)
        xlo_ref[face, :] = out_ref[q, 0:36, 0:wide]
        xhi_ref[face, :] = out_ref[q, 180:216, last : last + wide]
        for x in range(ex):
            dst = slice(x * LANES, (x + 1) * LANES)
            lo = slice(x * wide, x * wide + LANES)
            hi = slice((x + 1) * wide - LANES, (x + 1) * wide)
            for i in range(6):
                ylo_ref[36 * q + 6 * i : 36 * q + 6 * i + 6, dst] = out_ref[q, 36 * i : 36 * i + 6, lo]
                yhi_ref[36 * q + 6 * i : 36 * q + 6 * i + 6, dst] = out_ref[q, 36 * i + 30 : 36 * i + 36, hi]


def edge_kernel(ey, xl_ref, xr_ref, lo_ref, hi_ref):
    last = (ey - 1) * LANES
    for x, ref in enumerate((xl_ref, xr_ref)):
        for q in range(5):
            at = slice((x * 5 + q) * 6, (x * 5 + q) * 6 + 6)
            lo_ref[at, :] = ref[36 * q : 36 * q + 6, 0:LANES]
            hi_ref[at, :] = ref[36 * q + 30 : 36 * q + 36, last : last + LANES]


def finish_kernel(ex, ey, part_ref, xl_ref, xr_ref, yl_ref, yr_ref, el_ref, er_ref, out_ref, work):
    for q in range(5):
        for at in range(ex * ey):
            work[at] = part_ref[q, :, at * LANES : (at + 1) * LANES]
        for y in range(ey):
            lanes = slice(y * LANES, (y + 1) * LANES)
            work[y, 0:36, :] += xl_ref[36 * q : 36 * q + 36, lanes]
            work[(ex - 1) * ey + y, 180:216, :] += xr_ref[36 * q : 36 * q + 36, lanes]
        for x in range(ex):
            lanes = slice(x * LANES, (x + 1) * LANES)
            for i in range(6):
                work[x * ey, 36 * i : 36 * i + 6, :] += yl_ref[36 * q + 6 * i : 36 * q + 6 * i + 6, lanes]
                work[x * ey + ey - 1, 36 * i + 30 : 36 * i + 36, :] += yr_ref[36 * q + 6 * i : 36 * q + 6 * i + 6, lanes]
        for x in range(2):
            start, at = 180 * x, x * (ex - 1) * ey
            edge = slice((x * 5 + q) * 6, (x * 5 + q) * 6 + 6)
            work[at, start : start + 6, :] += el_ref[edge, :]
            work[at + ey - 1, start + 30 : start + 36, :] += er_ref[edge, :]
        for x in range(ex):
            for y in range(ey):
                at = x * ey + y
                lower = work[at, pl.ds(0, 36, stride=6), :]
                upper = work[at, pl.ds(5, 36, stride=6), :]
                work[at, pl.ds(5, 36, stride=6), :] = upper + pltpu.roll(lower, LANES - 1, 1)
                work[at, pl.ds(0, 36, stride=6), :] = lower + pltpu.roll(upper, 1, 1)
                out_ref[pl.ds((x * 5 + q) * NODES * ey + y, NODES, stride=ey), :] = work[at]


def call(kernel, out_shape, scratch=(), smem=0, late=0, hbm=(), flops=0, operands=()):
    spaces = [pltpu.SMEM if at < smem else pltpu.VMEM for at in range(len(operands))]
    if late:
        spaces[late] = pl.ANY
    for at in hbm:
        spaces[at] = pltpu.HBM
    return pl.pallas_call(
        kernel,
        out_shape=out_shape,
        in_specs=[pl.BlockSpec(memory_space=space) for space in spaces],
        out_specs=jax.tree.map(lambda s: pl.BlockSpec(memory_space=pltpu.VMEM), out_shape),
        scratch_shapes=list(scratch),
        cost_estimate=pl.CostEstimate(
            flops=flops, bytes_accessed=sum(x.size * 4 for x in operands), transcendentals=0
        ),
        compiler_params=pltpu.CompilerParams(vmem_limit_bytes=16 << 20),
    )(*operands)


def shape(*dims, dtype=F32):
    return jax.ShapeDtypeStruct(dims, dtype)


def step(rho, flow, hot, parent, count, basis, speed, breadth, heat):
    ex, ey, height = rho.shape[0], rho.shape[1], rho.shape[-1]
    elems = ex * ey * height
    groups, spans = lax.axis_size("gx"), lax.axis_size("gy")
    bins = parent.shape[0]
    half = bins // CHUNKS
    cap = bins // 4 // CHUNKS
    slots_t = basis.shape[-1]
    rows = -(-5 * NODES // 32) * 8
    me = lax.axis_index("gx").astype(I32).reshape(1)

    own = parent.reshape(1, bins)
    firsts = jnp.sum(
        (own // elems < jnp.arange(groups + 1, dtype=I32)[:, None]).astype(I32), axis=1
    )

    def swap(x, by):
        return lax.ppermute(x, "gx", [(i, i ^ by) for i in range(groups)])

    def exchange(x):
        return lax.all_to_all(x, "gx", 0, 0, tiled=True)

    def send(c, blocks):
        if WHOLE[c]:
            return [exchange(blocks[0])]
        got = {s: swap(blocks[s], s) for s in range(groups - 1, 0, -1)}
        return [blocks[0]] + [got[s] for s in range(1, groups)]

    ids = exchange(jnp.broadcast_to(own, (groups, bins)))
    rho_v = rho.transpose(0, 2, 3, 4, 1, 5).reshape(-1, height)
    flow_v = flow.transpose(0, 2, 3, 4, 5, 1, 6).reshape(-1, height)
    hot_v = hot.transpose(0, 2, 3, 4, 1, 5).reshape(-1, height)
    basis_v = basis.transpose(1, 2, 0, 3).reshape(18, bins, slots_t)
    speed_v = speed.transpose(1, 0, 2)

    def turn_y(x, by):
        return lax.ppermute(x, "gy", [(i, (i + by) % spans) for i in range(spans)])

    high, low = call(
        functools.partial(split_kernel, ex, ey),
        [shape(5 * NODES, elems, dtype=BF16)] * 2,
        [pltpu.VMEM(x.shape, F32) for x in (rho_v, flow_v, hot_v)] + [pltpu.SemaphoreType.DMA((3,))],
        hbm=(0, 1, 2),
        flops=10_000_000,
        operands=(rho_v, flow_v, hot_v),
    )
    arranged = call(
        functools.partial(arrange_kernel, elems, groups),
        [shape(23, slots_t, half)] * CHUNKS + [shape(8, half, dtype=I32)] * CHUNKS,
        flops=10_000_000,
        operands=(own, count.reshape(1, bins), basis_v, speed_v, breadth, heat),
    )
    data, live = arranged[:CHUNKS], arranged[CHUNKS:]
    states, wanted = [], []
    for c in range(CHUNKS):
        blocks = [shape(groups, rows, 4 * cap)] if WHOLE[c] else [shape(rows, 4 * cap)] * groups
        *wire, req = call(
            functools.partial(gather_kernel, c, elems, groups),
            blocks + [shape(groups * cap, LANES, dtype=I32)],
            [pltpu.VMEM((4 * rows, groups * cap), F32)],
            smem=1,
            late=4,
            flops=10_000_000,
            operands=(me, ids, high, low, ids if c == 0 else wanted[0]),
        )
        states.append(send(c, wire))
        wanted.append(req)
    fluid = call(
        functools.partial(fluid_kernel, ex, ey),
        shape(5, NODES, elems),
        [
            pltpu.VMEM((5, NODES, elems), F32),
            pltpu.VMEM((3, NODES, elems), F32),
            pltpu.VMEM((NODES, elems), F32),
        ],
        flops=10_000_000,
        operands=(jnp.asarray(gll_operator()), rho_v, flow_v, hot_v),
    )
    given = []
    after = wanted[1]
    for c in range(CHUNKS):
        wire = call(
            functools.partial(particle_kernel, c, groups),
            [shape(groups, NODES, 4 * cap)] if WHOLE[c] else [shape(NODES, 4 * cap)] * groups,
            [
                pltpu.VMEM((4 * rows, half), F32),
                pltpu.VMEM((4 * NODES, half), F32),
                pltpu.VMEM((4, slots_t, half), F32),
            ],
            smem=2,
            late=4,
            flops=20_000_000,
            operands=(me, firsts, data[c], live[c], after, *states[c]),
        )
        after = wire[0]
        given.append(send(c, wire))
    part = call(
        functools.partial(load_kernel, groups),
        shape(5, NODES, elems),
        flops=5_000_000,
        operands=(*given[0], wanted[0], fluid),
    )
    part, xlo, xhi, ylo, yhi = call(
        functools.partial(join_kernel, groups, ex, ey),
        (
            shape(5, NODES, elems),
            shape(180, ey * height),
            shape(180, ey * height),
            shape(180, ex * height),
            shape(180, ex * height),
        ),
        flops=5_000_000,
        operands=(*given[1], wanted[1], part),
    )
    xl = lax.ppermute(xhi, "gx", [(i, i + 1) for i in range(groups - 1)])
    xr = lax.ppermute(xlo, "gx", [(i + 1, i) for i in range(groups - 1)])
    yl, yr = turn_y(yhi, 1), turn_y(ylo, -1)
    elo, ehi = call(functools.partial(edge_kernel, ey), [shape(60, height)] * 2, flops=1_000_000, operands=(xl, xr))
    el, er = turn_y(ehi, 1), turn_y(elo, -1)
    out = call(
        functools.partial(finish_kernel, ex, ey),
        shape(ex * 5 * NODES * ey, height),
        [pltpu.VMEM((ex * ey, NODES, height), F32)],
        flops=5_000_000,
        operands=(part, xl, xr, yl, yr, el, er),
    )
    out = out.reshape(ex, 5, 6, 6, 6, ey, height)
    return out.transpose(0, 5, 1, 2, 3, 4, 6)


def solution(mesh):
    placed = (
        P("gx", "gy", None, None, None, None),
        P("gx", "gy", None, None, None, None, None),
        P("gx", "gy", None, None, None, None),
        P(("gx", "gy")),
        P(("gx", "gy")),
        P(("gx", "gy"), None, None, None),
        P(("gx", "gy"), None, None),
        P(("gx", "gy"), None),
        P(("gx", "gy"), None),
    )
    return jax.shard_map(
        step,
        mesh=mesh,
        in_specs=placed,
        out_specs=P("gx", "gy", None, None, None, None, None),
        check_vma=False,
    )
```
